256 devices in a mesh: row: 32 (over y, z_hi, x), col: 8 (over z_lo, core).
Axes of the slice: x: 4, y: 4, z: 8 (z_hi: 2, z_lo: 4; z = z_hi * 4 + z_lo), core: 2. Of those that a mesh axis runs over, the one named last changes fastest.
Arguments:
- top_tensor: bfloat16 [2304, 2304], P('row', 'col'), may hold values from -3 to 3
- bottom_tensor: bfloat16 [2304, 2304], P(('col', 'row')), may hold values from -3 to 3
- left_proj: bfloat16 [2304, 48], replicated, may hold values from -0.125 to 0.125
- right_proj: bfloat16 [2304, 48], replicated, may hold values from -0.125 to 0.125
Outputs:
- coarse: bfloat16 [2304, 2304], P(('col', 'row'))
The draws below stay inside these ranges and needn't reach their ends.
All inputs are finite; a program needn't handle non-finite values.
Results may differ from the reference program's by a relative error of at most 0.0065.
Values may be sent and summed in bfloat16 or wider, within the bound.
A program may use at most 128 MiB of HBM per device.

```python
import jax
import jax.numpy as jnp
from jax import lax

CHI = 48
N_COL = 8


def block_scale(stream_key, shape, pieces, smallest, largest):
    def one(dim, shards_of):
        heights = jax.random.uniform(jax.random.fold_in(jax.random.fold_in(stream_key, 6), dim), (shards_of,), jnp.float32, smallest / len(pieces), largest / len(pieces))
        return jnp.repeat(jnp.exp(heights), shape[dim] // shards_of).reshape((-1,) + (1,) * (len(shape) - dim - 1))

    level = one(*pieces[0])
    for cut in pieces[1:]:
        level = level * one(*cut)
    return level


def bell_draw(stream_key, shape, spread, limit, pieces=(), kind=jnp.bfloat16):
    result = jax.random.normal(stream_key, shape, jnp.float32) * spread
    if len(pieces) > 0:
        result = block_scale(stream_key, shape, pieces, -0.22, 0.18) * result
    return jnp.clip(result, min=-limit, max=limit).astype(kind)


def setup_inputs(seed: int = 0) -> dict:
    keys = jax.random.split(jax.random.key(seed), 5)
    return {
        "top_tensor": bell_draw(keys[0], (CHI * CHI, CHI * CHI), 0.38, 3.0, ((0, 32), (1, 8))),
        "bottom_tensor": bell_draw(keys[1], (CHI * CHI, CHI * CHI), 0.38, 3.0, ((0, 256),)),
        "left_proj": bell_draw(keys[2], (CHI * CHI, CHI), (CHI * CHI) ** -0.5, 0.125),
        "right_proj": bell_draw(keys[3], (CHI * CHI, CHI), (CHI * CHI) ** -0.5, 0.125),
    }


def reference(top_tensor, bottom_tensor, left_proj, right_proj):
    bond_dim = CHI
    block_len = CHI // N_COL
    left_table = left_proj.reshape(bond_dim, bond_dim, bond_dim).astype(jnp.float32)
    upper_part = top_tensor.reshape(bond_dim, bond_dim, bond_dim, bond_dim)

    def one_up(upper_slice):
        weighted = jnp.einsum("rml,lka->ramk", upper_slice.astype(jnp.float32), left_table, precision=lax.Precision.HIGHEST)
        weighted = weighted.astype(jnp.bfloat16).reshape(bond_dim * bond_dim, bond_dim * bond_dim)
        running = jnp.zeros((bond_dim * bond_dim, bond_dim), jnp.float32)
        for block_idx in range(N_COL):
            first = block_idx * block_len * bond_dim
            last = first + block_len * bond_dim
            paired = jnp.dot(weighted[:, first:last], bottom_tensor[first:last], preferred_element_type=jnp.float32)
            paired = paired.astype(jnp.bfloat16).reshape(bond_dim, bond_dim, bond_dim, bond_dim)
            paired = paired.transpose(1, 2, 0, 3).reshape(bond_dim * bond_dim, bond_dim * bond_dim)
            running = running + jnp.dot(paired, right_proj, preferred_element_type=jnp.float32)
        return running.reshape(bond_dim, bond_dim, bond_dim)

    per_up = lax.map(one_up, upper_part)
    coarse = per_up.transpose(2, 1, 0, 3).reshape(bond_dim * bond_dim, bond_dim * bond_dim)
    return coarse.astype(jnp.bfloat16)
```

```python
import jax
import jax.numpy as jnp
from jax import lax
from jax.experimental import pallas as pl
from jax.experimental.pallas import tpu as pltpu
from jax.sharding import PartitionSpec as P

CHI = 48
LANES = 256
PIECE = 16
GROUPS = 10
STEPS = 12


def spread_columns(x):
    lead = x.shape[:-1]
    x = x.reshape(*lead, 8, 6, CHI)
    none = [(0, 0, 0)] * len(lead)
    zero = jnp.zeros((), x.dtype)
    main = x[..., :5, :].reshape(*lead, 8, 5 * CHI)
    main = lax.pad(main, zero, none + [(0, 0, 0), (0, LANES - 5 * CHI, 0)])
    rest = x[..., 5, :].reshape(*lead, 2, 2, 2 * CHI)
    rest = lax.pad(rest, zero, none + [(0, 0, 0), (0, 0, 0), (0, CHI, 0)])
    rest = rest.reshape(*lead, 2, 6 * CHI)[..., :LANES]
    return jnp.concatenate([main, rest], axis=-2)


def left_placing(rows_here):
    lane = jnp.arange(LANES)
    n = lane // PIECE * rows_here + lane % PIECE
    valid = lane % PIECE < rows_here
    l2 = n % CHI
    return ((jnp.arange(CHI)[:, None] == l2[None, :]) & valid[None, :]).astype(jnp.bfloat16)


def right_placing():
    lane = jnp.arange(LANES)
    return (
        (jnp.arange(CHI)[:, None] == (lane % CHI)[None, :]) & (lane < 5 * CHI)[None, :]
    ).astype(jnp.bfloat16)


def f32dot(a, b):
    return jnp.dot(a, b, preferred_element_type=jnp.float32)


def compute_kernel(t1_ref, t2_ref, pl_ref, pr_ref, f_ref, g_ref, out_ref, plt, prt, wf, yb, acc):
    rows_here = 9
    plt[...] = f32dot(pl_ref[...], f_ref[...]).astype(jnp.bfloat16)
    prt[...] = f32dot(pr_ref[...], g_ref[...]).astype(jnp.bfloat16)
    lane = lax.broadcasted_iota(jnp.int32, (CHI, LANES), 1)
    n = lane // PIECE * rows_here + lane % PIECE
    t1 = t1_ref[...]
    zero = jnp.zeros((CHI, LANES), jnp.bfloat16)

    def weigh(a, _):
        w = plt[pl.ds(pl.multiple_of(a * CHI, CHI), CHI), :]
        block = jnp.concatenate(
            [jnp.where((n >= CHI * m) & (n < CHI * (m + 1)), w, zero) for m in range(3)], axis=0
        )
        r = f32dot(t1, block)
        for q in range(4):
            wf[q, pl.ds(a, 72, stride=CHI), :] = r[q // 2 * 72 : q // 2 * 72 + 72, q % 2 * 128 : q % 2 * 128 + 128]
        return _

    lax.fori_loop(0, CHI, weigh, 0)
    acc[...] = jnp.zeros_like(acc)
    p = lax.rem(lax.axis_index("row"), 2)

    def diag(r):
        w = prt[pl.ds(pl.multiple_of(r * CHI, CHI), CHI), :]
        parts = [
            jnp.where((lane >= CHI * e) & (lane < CHI * (e + 1)), w, zero) for e in range(5)
        ]
        return jnp.concatenate(parts + [zero[:16]], axis=0)

    def step(it, _):
        w = jnp.concatenate(
            [wf[q, pl.ds(pl.multiple_of(it * 288, 288), 288), :] for q in range(4)], axis=1
        ).astype(jnp.bfloat16)
        for g in range(GROUPS):
            yb[g] = f32dot(w, t2_ref[:, g * LANES : (g + 1) * LANES]).astype(jnp.bfloat16)
        first = 2 * it + 24 * p
        for start, size, shift in ((0, 96, 0), (96, 48, 24)):
            r = lax.rem(first + shift, CHI)
            weights = jnp.concatenate([diag(r), diag(r + 1)], axis=0)
            left = jnp.concatenate(
                [
                    yb[:, start : start + size, :].reshape(GROUPS * size, LANES),
                    yb[:, 144 + start : 144 + start + size, :].reshape(GROUPS * size, LANES),
                ],
                axis=1,
            )
            z = f32dot(left, weights).reshape(GROUPS, size, LANES)
            acc[:, start : start + size, :] += z
        return _

    lax.fori_loop(0, STEPS, step, 0)
    mid = acc[:, 96:144, :]
    none = jnp.zeros_like(mid)
    out_ref[:, 0:48, :] = (acc[:, 0:48, :] + jnp.where(p == 0, mid, none)).astype(jnp.bfloat16)
    out_ref[:, 48:96, :] = (acc[:, 48:96, :] + jnp.where(p == 0, none, mid)).astype(jnp.bfloat16)


def compute(t1, t2, plr, pr):
    return pl.pallas_call(
        compute_kernel,
        out_shape=jax.ShapeDtypeStruct((GROUPS, 96, LANES), jnp.bfloat16),
        in_specs=[pl.BlockSpec(memory_space=pltpu.VMEM)] * 6,
        out_specs=pl.BlockSpec(memory_space=pltpu.VMEM),
        scratch_shapes=[
            pltpu.VMEM((CHI * CHI, LANES), jnp.bfloat16),
            pltpu.VMEM((CHI * CHI, LANES), jnp.bfloat16),
            pltpu.VMEM((4, 72 * CHI, 128), jnp.float32),
            pltpu.VMEM((GROUPS, 288, LANES), jnp.bfloat16),
            pltpu.VMEM((GROUPS, 144, LANES), jnp.float32),
        ],
        compiler_params=pltpu.CompilerParams(vmem_limit_bytes=56 * 1024 * 1024),
    )(t1, t2, plr, pr, left_placing(9), right_placing())


def local(top_tensor, bottom_tensor, left_proj, right_proj):
    t1 = top_tensor.reshape(3, 24, 2, 144)
    t1 = jnp.stack([t1[0], t1[2], t1[1]], axis=1)
    t1 = t1.transpose(2, 0, 1, 3).reshape(144, 144)
    plr = left_proj.reshape(CHI, CHI, CHI).transpose(2, 0, 1).reshape(CHI * CHI, CHI)

    t2 = spread_columns(bottom_tensor).reshape(9, GROUPS * LANES)
    t2 = lax.all_gather(t2, "row", axis=0)
    t2 = lax.pad(t2, jnp.zeros((), t2.dtype), [(0, 0, 0), (0, PIECE - 9, 0), (0, 0, 0)])
    t2 = t2.reshape(32 * PIECE, GROUPS * LANES)

    part = compute(t1, t2, plr, right_proj)

    main = part[:8, :, : 5 * CHI].reshape(8, 2, CHI, 5, CHI)
    rest = lax.pad(part[8:], jnp.zeros((), part.dtype), [(0, 0, 0), (0, 0, 0), (0, 32, 0)])
    rest = rest.reshape(2, 96, 2, 144)[..., :96].reshape(2, 96, 2, 2, CHI)
    rest = rest.transpose(0, 2, 3, 1, 4).reshape(8, 2, CHI, 1, CHI)
    per_col = jnp.concatenate([main, rest], axis=3)
    got = lax.all_to_all(per_col, "col", 0, 0, tiled=True)
    summed = jnp.sum(got.astype(jnp.float32), axis=0)
    summed = summed.transpose(2, 1, 0, 3).reshape(288, 96)
    arrived = lax.all_to_all(summed.reshape(32, 9, 96), "row", 0, 0, tiled=True)
    arrived = arrived.reshape(16, 2, 9, 2, CHI)
    out = jnp.stack(
        [arrived[:, 0, :, 0], arrived[:, 0, :, 1] + arrived[:, 1, :, 0], arrived[:, 1, :, 1]], axis=1
    )
    return out.transpose(2, 0, 1, 3).reshape(9, CHI * CHI).astype(jnp.bfloat16)


def solution(mesh):
    return jax.shard_map(
        local,
        mesh=mesh,
        in_specs=(P("row", "col"), P(("col", "row"), None), P(), P()),
        out_specs=P(("col", "row"), None),
        check_vma=False,
    )
```

```python
import jax
import jax.numpy as jnp
from jax import lax
from jax.experimental import pallas as pl
from jax.experimental.pallas import tpu as pltpu
from jax.sharding import PartitionSpec as P

CHI = 48
LANES = 256
PIECE = 16
ROWS = 9
GROUPS = 5
STEPS = 12
PEERS = 32
SENDS = 128
MESH = pl.DeviceIdType.MESH
BF16 = jnp.bfloat16
SLOTS = (0, 1, 3, 4)


def spread_columns(x):
    x = x.reshape(ROWS, 4, 2, 6, CHI).transpose(2, 1, 0, 3, 4)
    zero = jnp.zeros((), x.dtype)
    none = (0, 0, 0)
    main = x[:, :, :, :5].reshape(2, 4, ROWS, 5 * CHI)
    main = lax.pad(main, zero, [none, none, none, (0, LANES - 5 * CHI, 0)])
    rest = x[:, :, :, 5].transpose(0, 2, 1, 3).reshape(2, ROWS, 2, 2 * CHI)
    rest = lax.pad(rest, zero, [none, none, none, (0, CHI, 0)])
    rest = rest.reshape(2, 1, ROWS, 6 * CHI)[..., :LANES]
    both = jnp.concatenate([main, rest], axis=1).reshape(2, GROUPS * ROWS, LANES)
    return lax.pad(both, zero, [none, (0, 48 - GROUPS * ROWS, 0), none])


def left_placing():
    lane = jnp.arange(LANES)
    n = lane // PIECE * ROWS + lane % PIECE
    valid = lane % PIECE < ROWS
    return ((jnp.arange(CHI)[:, None] == (n % CHI)[None, :]) & valid[None, :]).astype(BF16)


def right_placing():
    lane = jnp.arange(LANES)
    hit = jnp.arange(CHI)[:, None] == (lane % CHI)[None, :]
    return (hit & (lane < 5 * CHI)[None, :]).astype(BF16)


def row_window(g):
    return min(ROWS * g // 16 * 16, 16)


def row_placing():
    out = []
    to = jnp.arange(8 * PIECE)
    source = jnp.arange(8 * 32)
    for g in range(GROUPS):
        wanted = to // PIECE * 32 + ROWS * g - row_window(g) + to % PIECE
        hit = (wanted[:, None] == source[None, :]) & (to % PIECE < ROWS)[:, None]
        out.append(hit.astype(BF16))
    return jnp.stack(out)


def f32dot(a, b):
    return jnp.dot(a, b, preferred_element_type=jnp.float32)


def kernel(
    t1_ref, t2_ref, pl_ref, pr_ref, f_ref, g_ref, s_ref, out_ref,
    plt, prt, wf, yb, acc, t1s, pieces, t2p, part, extra, from_z, extra_z, rows, ready, arrived,
    sent, t1_got, piece_got, z_got, extra_got, row_got,
):
    i = lax.axis_index("row")
    j = lax.axis_index("col")
    x, zh, y = lax.rem(i, 4), lax.rem(i // 4, 2), i // 8
    core, zl = lax.rem(j, 2), j // 2
    other = 1 - core
    twin = 2 * zl + other

    barrier = pltpu.get_barrier_semaphore()
    for k in range(1, PEERS):
        pl.semaphore_signal(
            barrier, inc=1, device_id={"row": lax.rem(i + k, PEERS)}, device_id_type=MESH
        )
    pl.semaphore_signal(barrier, inc=1, device_id={"col": twin}, device_id_type=MESH)
    zpeers = [(lax.rem(zl + k, 4), 2 * lax.rem(zl + k, 4) + core) for k in range(1, 4)]
    for _, col in zpeers:
        pl.semaphore_signal(barrier, inc=1, device_id={"col": col}, device_id_type=MESH)

    plt[...] = f32dot(pl_ref[...], f_ref[...]).astype(BF16)
    prt[...] = f32dot(pr_ref[...], g_ref[...]).astype(BF16)
    acc[...] = jnp.zeros_like(acc)
    t1s[core] = t1_ref[...]
    pieces[i, core] = t2_ref[core]

    pl.semaphore_wait(barrier, PEERS - 1 + 1 + 3)

    copies = []

    def send(src, dst, got, where):
        copy = pltpu.make_async_remote_copy(
            src_ref=src, dst_ref=dst, send_sem=sent.at[len(copies)], recv_sem=got,
            device_id=where, device_id_type=MESH,
        )
        copy.start()
        copies.append(copy)

    def await_copy(ref, got):
        pltpu.make_async_remote_copy(
            src_ref=ref, dst_ref=ref, send_sem=sent.at[0], recv_sem=got,
            device_id={"col": twin}, device_id_type=MESH,
        ).wait_recv()

    def row_of(dz, dy, dx):
        return (lax.rem(y + dy, 4) * 2 + lax.rem(zh + dz, 2)) * 4 + lax.rem(x + dx, 4)

    def place(cr, dz, a, b):
        return row_of(dz, b, a) if cr == 0 else row_of(dz, a, b)

    def block(cr):
        return core if cr == 0 else other

    def pass_on(cr, dz, a, b, to_z=(), to_a=(), to_b=()):
        source, c = place(cr, dz, a, b), block(cr)
        own = cr == 0 and dz == 0 and a == 0 and b == 0
        src = t2_ref.at[core] if own else pieces.at[source, c]
        targets = [place(cr, 1, 0, 0) for _ in to_z]
        targets += [place(cr, 0, t, 0) for t in to_a] + [place(cr, 0, 0, t) for t in to_b]
        for target in targets:
            send(src, pieces.at[source, c], piece_got.at[source, c], {"row": target})

    def await_piece(cr, dz, a, b):
        source, c = place(cr, dz, a, b), block(cr)
        await_copy(pieces.at[source, c], piece_got.at[source, c])

    lane = lax.broadcasted_iota(jnp.int32, (CHI, LANES), 1)
    n = lane // PIECE * ROWS + lane % PIECE
    zero = jnp.zeros((CHI, LANES), BF16)

    def weigh(a, _):
        w = plt[pl.ds(pl.multiple_of(a * CHI, CHI), CHI), :]
        weights = jnp.concatenate(
            [jnp.where((n >= CHI * m) & (n < CHI * (m + 1)), w, zero) for m in range(3)], axis=0
        )
        r = f32dot(t1s[...].reshape(288, 144), weights)
        for t in range(4):
            for h in range(2):
                wf[2 * t + h, pl.ds(a, 72, stride=CHI), :] = r[
                    72 * t : 72 * t + 72, 128 * h : 128 * h + 128
                ]
        return _

    done = [0]

    def weigh_some(count):
        lax.fori_loop(done[0], done[0] + count, weigh, 0)
        done[0] += count

    send(t2_ref.at[other], pieces.at[i, core], piece_got.at[i, core], {"col": twin})
    send(t1_ref, t1s.at[core], t1_got, {"col": twin})
    pass_on(0, 0, 0, 0, to_z=(1,), to_a=(1, 3), to_b=(1, 3))
    await_piece(1, 0, 0, 0)
    pass_on(1, 0, 0, 0, to_z=(1,), to_a=(1, 3), to_b=(1, 3))
    await_copy(t1_ref, t1_got)
    weigh_some(8)

    def first_axis(dz):
        for cr in range(2):
            await_piece(cr, dz, 3, 0)
            pass_on(cr, dz, 3, 0, to_a=(1,) if dz == 0 else (), to_b=(1, 3))
            await_piece(cr, dz, 1, 0)
            pass_on(cr, dz, 1, 0, to_a=(3,) if dz == 1 else (), to_b=(1, 3))
        weigh_some(8)
        for cr in range(2):
            await_piece(cr, dz, 2, 0)
            pass_on(cr, dz, 2, 0, to_b=(1, 3))

    def second_axis(dz, a):
        for cr in range(2):
            await_piece(cr, dz, a, 3)
            if dz == 0:
                pass_on(cr, dz, a, 3, to_b=(1,))
            await_piece(cr, dz, a, 1)
            if dz == 1:
                pass_on(cr, dz, a, 1, to_b=(3,))

    def second_axis_end(dz, a):
        for cr in range(2):
            await_piece(cr, dz, a, 2)

    first_axis(0)
    for cr in range(2):
        await_piece(cr, 1, 0, 0)
        pass_on(cr, 1, 0, 0, to_a=(1, 3), to_b=(1, 3))
    second_axis(0, 0)
    weigh_some(8)
    second_axis(0, 3)
    second_axis(0, 1)
    first_axis(1)
    second_axis(0, 2)
    second_axis(1, 0)
    weigh_some(8)
    for a in (3, 1, 2):
        second_axis(1, a)
    weigh_some(8)
    for a in (0, 3, 1, 2):
        second_axis_end(0, a)
    for a in (0, 3, 1, 2):
        second_axis_end(1, a)

    for c in range(2):
        for k in range(4):
            for g in range(GROUPS):
                w = row_window(g)
                source = pieces[8 * k : 8 * k + 8, c, w : w + 32, :].reshape(256, LANES)
                t2p[512 * c + 128 * k : 512 * c + 128 * k + 128, LANES * g : LANES * g + LANES] = (
                    f32dot(s_ref[g], source).astype(BF16)
                )

    p = lax.rem(i, 2)

    def diag(r):
        w = prt[pl.ds(pl.multiple_of(r * CHI, CHI), CHI), :]
        parts = [
            jnp.where((lane >= CHI * e) & (lane < CHI * (e + 1)), w, zero) for e in range(5)
        ]
        return jnp.concatenate(parts + [zero[:16]], axis=0)

    def step(it, _):
        w = jnp.concatenate(
            [wf[q, pl.ds(pl.multiple_of(it * 288, 288), 288), :] for q in range(8)], axis=1
        ).astype(BF16)
        for g in range(GROUPS):
            yb[g] = f32dot(w, t2p[:, g * LANES : (g + 1) * LANES]).astype(BF16)
        first = 2 * it + 24 * p
        for start, size, shift in ((0, 96, 0), (96, 48, 24)):
            r = lax.rem(first + shift, CHI)
            weights = jnp.concatenate([diag(r), diag(r + 1)], axis=0)
            left = jnp.concatenate(
                [
                    yb[:, start : start + size, :].reshape(GROUPS * size, LANES),
                    yb[:, 144 + start : 144 + start + size, :].reshape(GROUPS * size, LANES),
                ],
                axis=1,
            )
            z = f32dot(left, weights).reshape(GROUPS, size, LANES)
            acc[:, start : start + size, :] += z
        return _

    lax.fori_loop(0, STEPS, step, 0)

    mid = acc[:, 96:144, :]
    none = jnp.zeros_like(mid)
    part[:, 0:48, :] = (acc[:, 0:48, :] + jnp.where(p == 0, mid, none)).astype(BF16)
    part[:, 48:96, :] = (acc[:, 48:96, :] + jnp.where(p == 0, none, mid)).astype(BF16)
    pad = jnp.zeros((CHI, 32), jnp.float32)
    last = part[4].astype(jnp.float32)
    for z in range(4):
        cut = slice(CHI * SLOTS[z], CHI * SLOTS[z] + CHI)
        extra[z] = jnp.concatenate([last[0:48, cut], last[48:96, cut], pad], axis=1).astype(BF16)
    for z, col in zpeers:
        send(part.at[z], from_z.at[zl], z_got.at[zl], {"col": col})
        send(extra.at[z], extra_z.at[zl], extra_got.at[zl], {"col": col})
    summed = part[zl].astype(jnp.float32)
    sixth = extra[zl].astype(jnp.float32)
    for z, _ in zpeers:
        await_copy(from_z.at[z], z_got.at[z])
        await_copy(extra_z.at[z], extra_got.at[z])
        summed += from_z[z].astype(jnp.float32)
        sixth += extra_z[z].astype(jnp.float32)
    for e in range(5):
        cut = slice(CHI * e, CHI * e + CHI)
        rows[CHI * e : CHI * e + CHI] = jnp.concatenate(
            [summed[0:48, cut], summed[48:96, cut], pad], axis=1
        )
    rows[240:288] = sixth
    rows[288:304] = jnp.zeros((16, 128), jnp.float32)
    for k in range(PEERS):
        ready[k] = rows[ROWS * k : ROWS * k + 16].astype(BF16)

    for k in range(1, PEERS):
        target = lax.rem(i + k, PEERS)
        send(ready.at[target], arrived.at[i], row_got.at[i], {"row": target})
    arrived[i] = ready[i]
    for k in range(1, PEERS):
        source = lax.rem(i + k, PEERS)
        await_copy(arrived.at[source], row_got.at[source])
    blocks = []
    for t in range(16):
        even, odd = arrived[2 * t].astype(jnp.float32), arrived[2 * t + 1].astype(jnp.float32)
        blocks += [even[:, 0:48], even[:, 48:96] + odd[:, 0:48], odd[:, 48:96]]
    out_ref[...] = jnp.concatenate(blocks, axis=1)[0:ROWS].astype(BF16)

    for copy in copies:
        copy.wait_send()


def local(top_tensor, bottom_tensor, left_proj, right_proj):
    t1 = top_tensor.reshape(3, 24, 2, 144)
    t1 = jnp.stack([t1[0], t1[2], t1[1]], axis=1)
    t1 = t1.transpose(2, 0, 1, 3).reshape(144, 144)
    plr = left_proj.reshape(CHI, CHI, CHI).transpose(2, 0, 1).reshape(CHI * CHI, CHI)
    t2 = spread_columns(bottom_tensor)
    dma = pltpu.SemaphoreType.DMA
    return pl.pallas_call(
        kernel,
        out_shape=jax.ShapeDtypeStruct((ROWS, CHI * CHI), BF16),
        in_specs=[pl.BlockSpec(memory_space=pltpu.VMEM)] * 7,
        out_specs=pl.BlockSpec(memory_space=pltpu.VMEM),
        scratch_shapes=[
            pltpu.VMEM((CHI * CHI, LANES), BF16),
            pltpu.VMEM((CHI * CHI, LANES), BF16),
            pltpu.VMEM((8, 72 * CHI, 128), jnp.float32),
            pltpu.VMEM((GROUPS, 288, LANES), BF16),
            pltpu.VMEM((GROUPS, 144, LANES), jnp.float32),
            pltpu.VMEM((2, 144, 144), BF16),
            pltpu.VMEM((PEERS, 2, 48, LANES), BF16),
            pltpu.VMEM((1024, GROUPS * LANES), BF16),
            pltpu.VMEM((GROUPS, 96, LANES), BF16),
            pltpu.VMEM((4, CHI, 128), BF16),
            pltpu.VMEM((4, 96, LANES), BF16),
            pltpu.VMEM((4, CHI, 128), BF16),
            pltpu.VMEM((304, 128), jnp.float32),
            pltpu.VMEM((PEERS, 16, 128), BF16),
            pltpu.VMEM((PEERS, 16, 128), BF16),
            dma((SENDS,)),
            dma,
            dma((PEERS, 2)),
            dma((4,)),
            dma((4,)),
            dma((PEERS,)),
        ],
        compiler_params=pltpu.CompilerParams(
            vmem_limit_bytes=60 * 1024 * 1024, collective_id=0, has_side_effects=True
        ),
    )(t1, t2, plr, right_proj, left_placing(), right_placing(), row_placing())


def solution(mesh):
    return jax.shard_map(
        local,
        mesh=mesh,
        in_specs=(P("row", "col"), P(("col", "row"), None), P(), P()),
        out_specs=P(("col", "row"), None),
        check_vma=False,
    )
```

```python
import jax
import jax.numpy as jnp
from jax import lax
from jax.experimental import pallas as pl
from jax.experimental.pallas import tpu as pltpu
from jax.sharding import PartitionSpec as P

CHI = 48
LANES = 256
PIECE = 16
ROWS = 9
GROUPS = 5
STEPS = 12
OUT = pltpu.VMEM((9, 2304), jnp.bfloat16)
PEERS = 32
SENDS = 128
MESH = pl.DeviceIdType.MESH
BF16 = jnp.bfloat16
SLOTS = (0, 1, 3, 4)


def row_window(g):
    return min(ROWS * g // 16 * 16, 16)


def f32dot(a, b):
    return jnp.dot(a, b, preferred_element_type=jnp.float32)


def one_hot(shape, hit):
    row = lax.broadcasted_iota(jnp.int32, shape, 0)
    col = lax.broadcasted_iota(jnp.int32, shape, 1)
    return jnp.where(hit(row, col), 1.0, 0.0).astype(BF16)


def kernel(
    t1_hbm, t2_hbm, pl_hbm, pr_hbm, out_ref,
    t1_ref, t2_ref, pl_ref, pr_ref, t1x, spread, t2s, plt, prt, wf, yb, acc, t1s, pieces, t2p,
    part, extra, from_z, extra_z, rows, ready, arrived,
    loaded, sent, t1_got, piece_got, z_got, extra_got, row_got,
):
    i = lax.axis_index("row")
    j = lax.axis_index("col")
    x, zh, y = lax.rem(i, 4), lax.rem(i // 4, 2), i // 8
    core, zl = lax.rem(j, 2), j // 2
    other = 1 - core
    twin = 2 * zl + other
    zpeers = [(lax.rem(zl + k, 4), 2 * lax.rem(zl + k, 4) + core) for k in range(1, 4)]

    def row_of(dz, dy, dx):
        return (lax.rem(y + dy, 4) * 2 + lax.rem(zh + dz, 2)) * 4 + lax.rem(x + dx, 4)

    loads = []
    for k, (src, dst) in enumerate(
        ((t2_hbm, t2_ref), (t1_hbm, t1_ref), (pl_hbm, pl_ref), (pr_hbm, pr_ref))
    ):
        loads.append(pltpu.make_async_copy(src, dst, loaded.at[k]))
        loads[-1].start()
    barrier = pltpu.get_barrier_semaphore()
    near = [row_of(0, 0, 1), row_of(0, 0, 3), row_of(0, 1, 0), row_of(0, 3, 0), row_of(1, 0, 0)]
    for peer in near:
        pl.semaphore_signal(barrier, inc=1, device_id={"row": peer}, device_id_type=MESH)
    for col in [twin] + [col for _, col in zpeers]:
        pl.semaphore_signal(barrier, inc=1, device_id={"col": col}, device_id_type=MESH)

    spread[...] = jnp.zeros_like(spread)
    loads[0].wait()
    t2 = t2_ref[...].astype(jnp.float32)
    for c in range(2):
        for z in range(4):
            at = 6 * CHI * (2 * z + c)
            spread[c, ROWS * z : ROWS * z + ROWS, 0 : 5 * CHI] = t2[:, at : at + 5 * CHI]
            slot = CHI * SLOTS[z]
            spread[c, 4 * ROWS : 5 * ROWS, slot : slot + CHI] = t2[:, at + 5 * CHI : at + 6 * CHI]
    t2s[...] = spread[...].astype(BF16)
    pieces[i, core] = t2s[core]
    loads[1].wait()

    pl.semaphore_wait(barrier, 5 + 1 + 3)

    copies = []

    def send(src, dst, got, where):
        copy = pltpu.make_async_remote_copy(
            src_ref=src, dst_ref=dst, send_sem=sent.at[len(copies)], recv_sem=got,
            device_id=where, device_id_type=MESH,
        )
        copy.start()
        copies.append(copy)

    def await_copy(ref, got):
        pltpu.make_async_remote_copy(
            src_ref=ref, dst_ref=ref, send_sem=sent.at[0], recv_sem=got,
            device_id={"col": twin}, device_id_type=MESH,
        ).wait_recv()

    def place(cr, dz, a, b):
        return row_of(dz, b, a) if cr == 0 else row_of(dz, a, b)

    def block(cr):
        return core if cr == 0 else other

    def pass_on(cr, dz, a, b, to_z=(), to_a=(), to_b=()):
        source, c = place(cr, dz, a, b), block(cr)
        own = cr == 0 and dz == 0 and a == 0 and b == 0
        src = t2s.at[core] if own else pieces.at[source, c]
        targets = [place(cr, 1, 0, 0) for _ in to_z]
        targets += [place(cr, 0, t, 0) for t in to_a] + [place(cr, 0, 0, t) for t in to_b]
        for target in targets:
            send(src, pieces.at[source, c], piece_got.at[source, c], {"row": target})

    def await_piece(cr, dz, a, b):
        source, c = place(cr, dz, a, b), block(cr)
        await_copy(pieces.at[source, c], piece_got.at[source, c])

    lane = lax.broadcasted_iota(jnp.int32, (CHI, LANES), 1)
    n = lane // PIECE * ROWS + lane % PIECE
    zero = jnp.zeros((CHI, LANES), BF16)
    swap = one_hot((192, 192), lambda r, c: (r // 8 == c % 24) & (r % 8 == c // 24))

    def weigh(ag, _):
        left = t1s[...]
        results = []
        for k in range(8):
            at = pl.multiple_of((8 * ag + k) * CHI, CHI)
            w = jnp.concatenate([plt[h, pl.ds(at, CHI), :] for h in range(2)], axis=1).astype(BF16)
            weights = jnp.concatenate(
                [jnp.where((n >= CHI * m) & (n < CHI * (m + 1)), w, zero) for m in range(3)], axis=0
            )
            results.append(f32dot(left, weights))
        for t in range(4):
            for s in range(3):
                at = 72 * t + 24 * s
                block = jnp.concatenate([r[at : at + 24] for r in results], axis=0).astype(BF16)
                turned = f32dot(swap, block)
                for q in range(24):
                    to = pl.multiple_of((24 * s + q) * CHI + 8 * ag, 8)
                    wf[pl.ds(to, 8), LANES * t : LANES * t + LANES] = turned[8 * q : 8 * q + 8]
        return _

    done = [0]

    def weigh_some(count):
        lax.fori_loop(done[0], done[0] + count, weigh, 0)
        done[0] += count

    send(t2s.at[other], pieces.at[i, core], piece_got.at[i, core], {"col": twin})
    send(t1_ref, t1x, t1_got, {"col": twin})
    pass_on(0, 0, 0, 0, to_z=(1,), to_a=(1, 3), to_b=(1, 3))
    await_piece(1, 0, 0, 0)
    pass_on(1, 0, 0, 0, to_z=(1,), to_a=(1, 3), to_b=(1, 3))

    place_left = one_hot(
        (CHI, LANES),
        lambda r, c: (r == (c // PIECE * ROWS + c % PIECE) % CHI) & (c % PIECE < ROWS),
    )
    place_right = one_hot((CHI, LANES), lambda r, c: (r == c % CHI) & (c < 5 * CHI))
    loads[2].wait()
    left_proj = pl_ref[...].astype(jnp.float32)
    for k in range(CHI):
        z = f32dot(left_proj[:, CHI * k : CHI * k + CHI].astype(BF16), place_left)
        for h in range(2):
            plt[h, pl.ds(k, CHI, stride=CHI), :] = z[:, 128 * h : 128 * h + 128]
    acc[...] = jnp.zeros_like(acc)
    await_copy(t1x, t1_got)
    mine, theirs = t1_ref[...].astype(jnp.float32), t1x[...].astype(jnp.float32)
    lower = jnp.where(core == 0, mine, theirs)
    upper = jnp.where(core == 0, theirs, mine)
    t1s[...] = jnp.concatenate(
        [lower[:, 0:144], lower[:, 144:288], upper[:, 0:144], upper[:, 144:288]], axis=0
    ).astype(BF16)

    def first_axis(dz):
        for cr in range(2):
            await_piece(cr, dz, 3, 0)
            pass_on(cr, dz, 3, 0, to_a=(1,) if dz == 0 else (), to_b=(1, 3))
            await_piece(cr, dz, 1, 0)
            pass_on(cr, dz, 1, 0, to_a=(3,) if dz == 1 else (), to_b=(1, 3))
        weigh_some(1)
        for cr in range(2):
            await_piece(cr, dz, 2, 0)
            pass_on(cr, dz, 2, 0, to_b=(1, 3))

    def second_axis(dz, a):
        for cr in range(2):
            await_piece(cr, dz, a, 3)
            if dz == 0:
                pass_on(cr, dz, a, 3, to_b=(1,))
            await_piece(cr, dz, a, 1)
            if dz == 1:
                pass_on(cr, dz, a, 1, to_b=(3,))

    def second_axis_end(dz, a):
        for cr in range(2):
            await_piece(cr, dz, a, 2)

    first_axis(0)
    for cr in range(2):
        await_piece(cr, 1, 0, 0)
        pass_on(cr, 1, 0, 0, to_a=(1, 3), to_b=(1, 3))
    second_axis(0, 0)
    weigh_some(1)
    second_axis(0, 3)
    second_axis(0, 1)
    first_axis(1)
    second_axis(0, 2)
    second_axis(1, 0)
    weigh_some(1)
    for a in (3, 1, 2):
        second_axis(1, a)
    weigh_some(1)
    for a in (0, 3, 1, 2):
        second_axis_end(0, a)
    for a in (0, 3, 1, 2):
        second_axis_end(1, a)

    weigh_some(1)
    loads[3].wait()
    prt[...] = lax.dot_general(
        pr_ref[...], place_right, (((0,), (0,)), ((), ())), preferred_element_type=jnp.float32
    ).astype(BF16)

    for g in range(GROUPS):
        w = row_window(g)
        pick = one_hot(
            (8 * PIECE, 256),
            lambda r, c: (c == r // PIECE * 32 + ROWS * g - w + r % PIECE) & (r % PIECE < ROWS),
        )
        for c in range(2):
            for k in range(4):
                source = pieces[8 * k : 8 * k + 8, c, w : w + 32, :].reshape(256, LANES)
                t2p[512 * c + 128 * k : 512 * c + 128 * k + 128, LANES * g : LANES * g + LANES] = (
                    f32dot(pick, source).astype(BF16)
                )

    p = lax.rem(i, 2)

    def diag(r):
        w = prt[pl.ds(pl.multiple_of(r * CHI, CHI), CHI), :]
        parts = [
            jnp.where((lane >= CHI * e) & (lane < CHI * (e + 1)), w, zero) for e in range(5)
        ]
        return jnp.concatenate(parts + [zero[:16]], axis=0)

    def step(it, _):
        starts = [pl.multiple_of((24 * s + 2 * it) * CHI, CHI) for s in (0, 2, 1)]
        w = jnp.concatenate([wf[pl.ds(at, 96), :] for at in starts], axis=0).astype(BF16)
        for g in range(GROUPS):
            yb[g] = f32dot(w, t2p[:, g * LANES : (g + 1) * LANES]).astype(BF16)
        first = 2 * it + 24 * p
        for to, parts, shift in ((0, (0, 96), 0), (96, (192,), 24)):
            r = lax.rem(first + shift, CHI)
            size = CHI * len(parts)
            weights = jnp.concatenate([diag(r), diag(r + 1)], axis=0)
            sides = []
            for k in range(2):
                side = [yb[:, at + CHI * k : at + CHI * k + CHI, :] for at in parts]
                sides.append(jnp.concatenate(side, axis=1).reshape(GROUPS * size, LANES))
            left = jnp.concatenate(sides, axis=1)
            z = f32dot(left, weights).reshape(GROUPS, size, LANES)
            acc[:, to : to + size, :] += z
        return _

    lax.fori_loop(0, STEPS, step, 0)

    mid = acc[:, 96:144, :]
    none = jnp.zeros_like(mid)
    part[:, 0:48, :] = (acc[:, 0:48, :] + jnp.where(p == 0, mid, none)).astype(BF16)
    part[:, 48:96, :] = (acc[:, 48:96, :] + jnp.where(p == 0, none, mid)).astype(BF16)
    pad = jnp.zeros((CHI, 32), jnp.float32)
    last = part[4].astype(jnp.float32)
    for z in range(4):
        cut = slice(CHI * SLOTS[z], CHI * SLOTS[z] + CHI)
        extra[z] = jnp.concatenate([last[0:48, cut], last[48:96, cut], pad], axis=1).astype(BF16)
    for z, col in zpeers:
        send(part.at[z], from_z.at[zl], z_got.at[zl], {"col": col})
        send(extra.at[z], extra_z.at[zl], extra_got.at[zl], {"col": col})
    summed = part[zl].astype(jnp.float32)
    sixth = extra[zl].astype(jnp.float32)
    for z, _ in zpeers:
        await_copy(from_z.at[z], z_got.at[z])
        await_copy(extra_z.at[z], extra_got.at[z])
        summed += from_z[z].astype(jnp.float32)
        sixth += extra_z[z].astype(jnp.float32)
    for e in range(5):
        cut = slice(CHI * e, CHI * e + CHI)
        rows[CHI * e : CHI * e + CHI] = jnp.concatenate(
            [summed[0:48, cut], summed[48:96, cut], pad], axis=1
        )
    rows[240:288] = sixth
    rows[288:304] = jnp.zeros((16, 128), jnp.float32)
    for k in range(PEERS):
        ready[k] = rows[ROWS * k : ROWS * k + 16].astype(BF16)

    for k in range(1, PEERS):
        target = lax.rem(i + k, PEERS)
        send(ready.at[target], arrived.at[i], row_got.at[i], {"row": target})
    arrived[i] = ready[i]
    for k in range(1, PEERS):
        source = lax.rem(i + k, PEERS)
        await_copy(arrived.at[source], row_got.at[source])
    blocks = []
    for t in range(16):
        even, odd = arrived[2 * t].astype(jnp.float32), arrived[2 * t + 1].astype(jnp.float32)
        blocks += [even[:, 0:48], even[:, 48:96] + odd[:, 0:48], odd[:, 48:96]]
    out_ref[...] = jnp.concatenate(blocks, axis=1)[0:ROWS].astype(BF16)

    for copy in copies:
        copy.wait_send()


def local(top_tensor, bottom_tensor, left_proj, right_proj):
    dma = pltpu.SemaphoreType.DMA
    return pl.pallas_call(
        kernel,
        out_shape=OUT,
        in_specs=[pl.BlockSpec(memory_space=pl.ANY)] * 4,
        out_specs=pl.BlockSpec(memory_space=pltpu.VMEM),
        scratch_shapes=[
            pltpu.VMEM((72, 288), BF16),
            pltpu.VMEM((ROWS, CHI * CHI), BF16),
            pltpu.VMEM((CHI, CHI * CHI), BF16),
            pltpu.VMEM((CHI, CHI * CHI), BF16),
            pltpu.VMEM((72, 288), BF16),
            pltpu.VMEM((2, 48, LANES), jnp.float32),
            pltpu.VMEM((2, 48, LANES), BF16),
            pltpu.VMEM((2, CHI * CHI, 128), jnp.float32),
            pltpu.VMEM((CHI * CHI, LANES), BF16),
            pltpu.VMEM((72 * CHI, 4 * LANES), jnp.float32),
            pltpu.VMEM((GROUPS, 288, LANES), BF16),
            pltpu.VMEM((GROUPS, 144, LANES), jnp.float32),
            pltpu.VMEM((288, 144), BF16),
            pltpu.VMEM((PEERS, 2, 48, LANES), BF16),
            pltpu.VMEM((1024, GROUPS * LANES), BF16),
            pltpu.VMEM((GROUPS, 96, LANES), BF16),
            pltpu.VMEM((4, CHI, 128), BF16),
            pltpu.VMEM((4, 96, LANES), BF16),
            pltpu.VMEM((4, CHI, 128), BF16),
            pltpu.VMEM((304, 128), jnp.float32),
            pltpu.VMEM((PEERS, 16, 128), BF16),
            pltpu.VMEM((PEERS, 16, 128), BF16),
            dma((4,)),
            dma((SENDS,)),
            dma,
            dma((PEERS, 2)),
            dma((4,)),
            dma((4,)),
            dma((PEERS,)),
        ],
        compiler_params=pltpu.CompilerParams(
            vmem_limit_bytes=60 * 1024 * 1024, collective_id=0, has_side_effects=True
        ),
    )(top_tensor, bottom_tensor, left_proj.T, right_proj.T)


def solution(mesh):
    return jax.shard_map(
        local,
        mesh=mesh,
        in_specs=(P("row", "col"), P(("col", "row"), None), P(), P()),
        out_specs=P(("col", "row"), None),
        check_vma=False,
    )
```

```python
import jax
import jax.numpy as jnp
from jax import lax
from jax.experimental import pallas as pl
from jax.experimental.pallas import tpu as pltpu
from jax.sharding import PartitionSpec as P

CHI = 48
LANES = 256
PIECE = 16
ROWS = 9
GROUPS = 5
NB = 4
OUT = pltpu.VMEM((9, 2304), jnp.bfloat16)
PEERS = 32
MESH = pl.DeviceIdType.MESH
BF16 = jnp.bfloat16
SLOTS = (0, 1, 3, 4)


def row_window(g):
    return min(ROWS * g // 16 * 16, 16)


def f32dot(a, b):
    return jnp.dot(a, b, preferred_element_type=jnp.float32)


def one_hot(shape, hit):
    row = lax.broadcasted_iota(jnp.int32, shape, 0)
    col = lax.broadcasted_iota(jnp.int32, shape, 1)
    return jnp.where(hit(row, col), 1.0, 0.0).astype(BF16)


def kernel(
    t1_hbm, t2_hbm, pl_hbm, pr_hbm, out_ref,
    t1_ref, t2_ref, pl_ref, pr_ref, t1x, spread, t2s, plt, prt, wf, yb, acc, t1s, pieces, t2p,
    part, extra, from_z, extra_z, rows, ready, arrived,
    loaded, sent, t1_got, piece_got, z_got, extra_got, row_got,
):
    i = lax.axis_index("row")
    j = lax.axis_index("col")
    x, zh, y = lax.rem(i, 4), lax.rem(i // 4, 2), i // 8
    core, zl = lax.rem(j, 2), j // 2
    other = 1 - core
    twin = 2 * zl + other
    zpeers = [(lax.rem(zl + k, 4), 2 * lax.rem(zl + k, 4) + core) for k in range(1, 4)]

    def row_of(dz, dy, dx):
        return (lax.rem(y + dy, 4) * 2 + lax.rem(zh + dz, 2)) * 4 + lax.rem(x + dx, 4)

    loads = []
    for k, (src, dst) in enumerate(
        ((t2_hbm, t2_ref), (t1_hbm, t1_ref), (pl_hbm, pl_ref), (pr_hbm, pr_ref))
    ):
        loads.append(pltpu.make_async_copy(src, dst, loaded.at[k]))
        loads[-1].start()
    barrier = pltpu.get_barrier_semaphore()
    near = [row_of(0, 0, 1), row_of(0, 0, 3), row_of(0, 1, 0), row_of(0, 3, 0), row_of(1, 0, 0)]
    for peer in near:
        pl.semaphore_signal(barrier, inc=1, device_id={"row": peer}, device_id_type=MESH)
    for col in [twin] + [col for _, col in zpeers]:
        pl.semaphore_signal(barrier, inc=1, device_id={"col": col}, device_id_type=MESH)

    spread[...] = jnp.zeros_like(spread)
    loads[0].wait()
    t2 = t2_ref[...].astype(jnp.float32)
    for c in range(2):
        for z in range(4):
            at = 6 * CHI * (2 * z + c)
            spread[c, ROWS * z : ROWS * z + ROWS, 0 : 5 * CHI] = t2[:, at : at + 5 * CHI]
            slot = CHI * SLOTS[z]
            spread[c, 4 * ROWS : 5 * ROWS, slot : slot + CHI] = t2[:, at + 5 * CHI : at + 6 * CHI]
    t2s[...] = spread[...].astype(BF16)
    pieces[i, core] = t2s[core]
    loads[1].wait()

    pl.semaphore_wait(barrier, 5 + 1 + 3)

    counts = [0] * 6

    def remote(src, dst, kind, got, where):
        return pltpu.make_async_remote_copy(
            src_ref=src, dst_ref=dst, send_sem=sent.at[kind], recv_sem=got,
            device_id=where, device_id_type=MESH,
        )

    def send(kind, src, dst, got, where):
        remote(src, dst, kind, got, where).start()
        counts[kind] += 1

    def await_copy(ref, got):
        remote(ref, ref, 0, got, {"col": twin}).wait_recv()

    def await_sent(kind, ref):
        remote(ref, ref, kind, t1_got, {"col": twin}).wait_send()

    def place(cr, dz, a, b):
        return row_of(dz, b, a) if cr == 0 else row_of(dz, a, b)

    def block(cr):
        return core if cr == 0 else other

    def pass_on(cr, dz, a, b, to_z=(), to_a=(), to_b=()):
        source, c = place(cr, dz, a, b), block(cr)
        own = cr == 0 and dz == 0 and a == 0 and b == 0
        src = t2s.at[core] if own else pieces.at[source, c]
        targets = [place(cr, 1, 0, 0) for _ in to_z]
        targets += [place(cr, 0, t, 0) for t in to_a] + [place(cr, 0, 0, t) for t in to_b]
        for target in targets:
            send(0, src, pieces.at[source, c], piece_got.at[source, c], {"row": target})

    def await_piece(cr, dz, a, b):
        source, c = place(cr, dz, a, b), block(cr)
        await_copy(pieces.at[source, c], piece_got.at[source, c])

    lane = lax.broadcasted_iota(jnp.int32, (CHI, LANES), 1)
    n = lane // PIECE * ROWS + lane % PIECE
    zero = jnp.zeros((CHI, LANES), BF16)
    swap = one_hot((192, 192), lambda r, c: (r // 8 == c % 24) & (r % 8 == c // 24))

    def weigh(ag, _):
        left = t1s[...]
        results = []
        for k in range(8):
            at = pl.multiple_of((8 * ag + k) * CHI, CHI)
            w = jnp.concatenate([plt[h, pl.ds(at, CHI), :] for h in range(2)], axis=1).astype(BF16)
            weights = jnp.concatenate(
                [jnp.where((n >= CHI * m) & (n < CHI * (m + 1)), w, zero) for m in range(3)], axis=0
            )
            results.append(f32dot(left, weights))
        for t in range(4):
            for s in range(3):
                at = 72 * t + 24 * s
                block = jnp.concatenate([r[at : at + 24] for r in results], axis=0).astype(BF16)
                turned = f32dot(swap, block)
                for q in range(24):
                    to = pl.multiple_of((24 * s + q) * CHI + 8 * ag, 8)
                    wf[pl.ds(to, 8), LANES * t : LANES * t + LANES] = turned[8 * q : 8 * q + 8]
        return _

    done = [0]

    def weigh_some(count):
        lax.fori_loop(done[0], done[0] + count, weigh, 0)
        done[0] += count

    send(5, t2s.at[other], pieces.at[i, core], piece_got.at[i, core], {"col": twin})
    send(1, t1_ref, t1x, t1_got, {"col": twin})
    pass_on(0, 0, 0, 0, to_z=(1,), to_a=(1, 3), to_b=(1, 3))
    await_piece(1, 0, 0, 0)
    pass_on(1, 0, 0, 0, to_z=(1,), to_a=(1, 3), to_b=(1, 3))

    place_left = one_hot(
        (CHI, LANES),
        lambda r, c: (r == (c // PIECE * ROWS + c % PIECE) % CHI) & (c % PIECE < ROWS),
    )
    place_right = one_hot((CHI, LANES), lambda r, c: (r == c % CHI) & (c < 5 * CHI))
    loads[2].wait()
    left_proj = pl_ref[...].astype(jnp.float32)
    for k in range(CHI):
        z = f32dot(left_proj[:, CHI * k : CHI * k + CHI].astype(BF16), place_left)
        for h in range(2):
            plt[h, pl.ds(k, CHI, stride=CHI), :] = z[:, 128 * h : 128 * h + 128]
    acc[...] = jnp.zeros_like(acc)
    await_copy(t1x, t1_got)
    mine, theirs = t1_ref[...].astype(jnp.float32), t1x[...].astype(jnp.float32)
    lower = jnp.where(core == 0, mine, theirs)
    upper = jnp.where(core == 0, theirs, mine)
    t1s[...] = jnp.concatenate(
        [lower[:, 0:144], lower[:, 144:288], upper[:, 0:144], upper[:, 144:288]], axis=0
    ).astype(BF16)

    def first_axis(dz):
        for cr in range(2):
            await_piece(cr, dz, 3, 0)
            pass_on(cr, dz, 3, 0, to_a=(1,) if dz == 0 else (), to_b=(1, 3))
            await_piece(cr, dz, 1, 0)
            pass_on(cr, dz, 1, 0, to_a=(3,) if dz == 1 else (), to_b=(1, 3))

    def first_axis_end(dz):
        for cr in range(2):
            await_piece(cr, dz, 2, 0)
            pass_on(cr, dz, 2, 0, to_b=(1, 3))

    def second_axis(dz, a):
        for cr in range(2):
            await_piece(cr, dz, a, 3)
            if dz == 0:
                pass_on(cr, dz, a, 3, to_b=(1,))
            await_piece(cr, dz, a, 1)
            if dz == 1:
                pass_on(cr, dz, a, 1, to_b=(3,))

    def second_axis_end(dz, a):
        for cr in range(2):
            await_piece(cr, dz, a, 2)

    def pack(dz):
        for g in range(GROUPS):
            w = row_window(g)
            pick = one_hot(
                (4 * PIECE, 128),
                lambda r, c: (c == r // PIECE * 32 + ROWS * g - w + r % PIECE) & (r % PIECE < ROWS),
            )
            for c in range(2):
                for k in range(4):
                    at = pl.multiple_of((2 * k + lax.rem(zh + dz, 2)) * 4, 4)
                    source = pieces[pl.ds(at, 4), c, w : w + 32, :].reshape(128, LANES)
                    to = pl.multiple_of(512 * c + PIECE * at, 64)
                    t2p[pl.ds(to, 64), LANES * g : LANES * g + LANES] = f32dot(
                        pick, source
                    ).astype(BF16)

    first_axis(0)
    weigh_some(1)
    first_axis_end(0)
    weigh_some(1)
    second_axis(0, 0)
    weigh_some(1)
    second_axis(0, 3)
    second_axis(0, 1)
    weigh_some(1)
    for cr in range(2):
        await_piece(cr, 1, 0, 0)
        pass_on(cr, 1, 0, 0, to_a=(1, 3), to_b=(1, 3))
    second_axis(0, 2)
    weigh_some(1)
    first_axis(1)
    weigh_some(1)
    first_axis_end(1)
    for a in (0, 3, 1, 2):
        second_axis_end(0, a)
    second_axis(1, 0)
    loads[3].wait()
    prt[...] = lax.dot_general(
        pr_ref[...], place_right, (((0,), (0,)), ((), ())), preferred_element_type=jnp.float32
    ).astype(BF16)
    for a in (3, 1):
        second_axis(1, a)
    pack(0)
    second_axis(1, 2)
    for a in (0, 3, 1, 2):
        second_axis_end(1, a)
    pack(1)

    p = lax.rem(i, 2)

    def diag(r):
        w = prt[pl.ds(pl.multiple_of(r * CHI, CHI), CHI), :]
        parts = [
            jnp.where((lane >= CHI * e) & (lane < CHI * (e + 1)), w, zero) for e in range(5)
        ]
        return jnp.concatenate(parts + [zero[:16]], axis=0)

    def step(it, _):
        size = NB * CHI
        starts = [pl.multiple_of((24 * s + NB * it) * CHI, CHI) for s in (0, 2, 1)]
        w = jnp.concatenate([wf[pl.ds(at, size), :] for at in starts], axis=0).astype(BF16)
        for g in range(GROUPS):
            yb[g] = f32dot(w, t2p[:, g * LANES : (g + 1) * LANES]).astype(BF16)
        first = NB * it + 24 * p
        for to, parts, shift in ((0, (0, 1), 0), (96, (2,), 24)):
            r = lax.rem(first + shift, CHI)
            rows_here = CHI * len(parts)
            weights = jnp.concatenate([diag(r + k) for k in range(NB)], axis=0)
            sides = []
            for k in range(NB):
                side = [yb[:, size * s + CHI * k : size * s + CHI * k + CHI, :] for s in parts]
                sides.append(jnp.concatenate(side, axis=1).reshape(GROUPS * rows_here, LANES))
            z = f32dot(jnp.concatenate(sides, axis=1), weights)
            acc[:, to : to + rows_here, :] += z.reshape(GROUPS, rows_here, LANES)
        return _

    lax.fori_loop(0, 24 // NB, step, 0)

    mid = acc[:, 96:144, :]
    none = jnp.zeros_like(mid)
    part[:, 0:48, :] = (acc[:, 0:48, :] + jnp.where(p == 0, mid, none)).astype(BF16)
    part[:, 48:96, :] = (acc[:, 48:96, :] + jnp.where(p == 0, none, mid)).astype(BF16)
    pad = jnp.zeros((CHI, 32), jnp.float32)
    last = part[4].astype(jnp.float32)
    for z in range(4):
        cut = slice(CHI * SLOTS[z], CHI * SLOTS[z] + CHI)
        extra[z] = jnp.concatenate([last[0:48, cut], last[48:96, cut], pad], axis=1).astype(BF16)
    for z, col in zpeers:
        send(2, part.at[z], from_z.at[zl], z_got, {"col": col})
        send(3, extra.at[z], extra_z.at[zl], extra_got, {"col": col})
    summed = part[zl].astype(jnp.float32)
    sixth = extra[zl].astype(jnp.float32)
    await_copy(from_z.at[0:3], z_got)
    await_copy(extra_z.at[0:3], extra_got)
    for z, _ in zpeers:
        summed += from_z[z].astype(jnp.float32)
        sixth += extra_z[z].astype(jnp.float32)
    for e in range(5):
        cut = slice(CHI * e, CHI * e + CHI)
        rows[CHI * e : CHI * e + CHI] = jnp.concatenate(
            [summed[0:48, cut], summed[48:96, cut], pad], axis=1
        )
    rows[240:288] = sixth
    rows[288:304] = jnp.zeros((16, 128), jnp.float32)
    for k in range(PEERS):
        ready[k] = rows[ROWS * k : ROWS * k + 16].astype(BF16)

    for k in range(1, PEERS):
        target = lax.rem(i + k, PEERS)
        send(4, ready.at[target], arrived.at[i], row_got, {"row": target})
    arrived[i] = ready[i]
    await_copy(arrived.at[0 : PEERS - 1], row_got)
    blocks = []
    for t in range(16):
        even, odd = arrived[2 * t].astype(jnp.float32), arrived[2 * t + 1].astype(jnp.float32)
        blocks += [even[:, 0:48], even[:, 48:96] + odd[:, 0:48], odd[:, 48:96]]
    out_ref[...] = jnp.concatenate(blocks, axis=1)[0:ROWS].astype(BF16)

    assert counts == [2 * (counts[0] // 2), 1, 3, 3, PEERS - 1, 1], counts
    await_sent(0, pieces.at[0 : counts[0] // 2])
    await_sent(5, t2s.at[0])
    await_sent(1, t1x)
    await_sent(2, from_z.at[0:3])
    await_sent(3, extra_z.at[0:3])
    await_sent(4, arrived.at[0 : PEERS - 1])


def local(top_tensor, bottom_tensor, left_proj, right_proj):
    dma = pltpu.SemaphoreType.DMA
    return pl.pallas_call(
        kernel,
        out_shape=OUT,
        in_specs=[pl.BlockSpec(memory_space=pl.ANY)] * 4,
        out_specs=pl.BlockSpec(memory_space=pltpu.VMEM),
        scratch_shapes=[
            pltpu.VMEM((72, 288), BF16),
            pltpu.VMEM((ROWS, CHI * CHI), BF16),
            pltpu.VMEM((CHI, CHI * CHI), BF16),
            pltpu.VMEM((CHI, CHI * CHI), BF16),
            pltpu.VMEM((72, 288), BF16),
            pltpu.VMEM((2, 48, LANES), jnp.float32),
            pltpu.VMEM((2, 48, LANES), BF16),
            pltpu.VMEM((2, CHI * CHI, 128), jnp.float32),
            pltpu.VMEM((CHI * CHI, LANES), BF16),
            pltpu.VMEM((72 * CHI, 4 * LANES), jnp.float32),
            pltpu.VMEM((GROUPS, 3 * NB * CHI, LANES), BF16),
            pltpu.VMEM((GROUPS, 144, LANES), jnp.float32),
            pltpu.VMEM((288, 144), BF16),
            pltpu.VMEM((PEERS, 2, 48, LANES), BF16),
            pltpu.VMEM((1024, GROUPS * LANES), BF16),
            pltpu.VMEM((GROUPS, 96, LANES), BF16),
            pltpu.VMEM((4, CHI, 128), BF16),
            pltpu.VMEM((4, 96, LANES), BF16),
            pltpu.VMEM((4, CHI, 128), BF16),
            pltpu.VMEM((304, 128), jnp.float32),
            pltpu.VMEM((PEERS, 16, 128), BF16),
            pltpu.VMEM((PEERS, 16, 128), BF16),
            dma((4,)),
            dma((6,)),
            dma,
            dma((PEERS, 2)),
            dma,
            dma,
            dma,
        ],
        compiler_params=pltpu.CompilerParams(
            vmem_limit_bytes=60 * 1024 * 1024, collective_id=0, has_side_effects=True
        ),
    )(top_tensor, bottom_tensor, left_proj.T, right_proj.T)


def solution(mesh):
    return jax.shard_map(
        local,
        mesh=mesh,
        in_specs=(P("row", "col"), P(("col", "row"), None), P(), P()),
        out_specs=P(("col", "row"), None),
        check_vma=False,
    )
```

```python
import jax
import jax.numpy as jnp
from jax import lax
from jax.experimental import pallas as pl
from jax.experimental.pallas import tpu as pltpu
from jax.sharding import PartitionSpec as P

CHI = 48
LANES = 256
ROWS = 9
TILE = 4 * CHI
GROUPS = 5
NB = 4
OUT = pltpu.VMEM((9, 2304), jnp.bfloat16)
PEERS = 32
MESH = pl.DeviceIdType.MESH
BF16 = jnp.bfloat16
SLOTS = (0, 1, 3, 4)


def row_window(g):
    return min(ROWS * g // 16 * 16, 16)


def f32dot(a, b):
    return jnp.dot(a, b, preferred_element_type=jnp.float32)


def one_hot(shape, hit):
    row = lax.broadcasted_iota(jnp.int32, shape, 0)
    col = lax.broadcasted_iota(jnp.int32, shape, 1)
    return jnp.where(hit(row, col), 1.0, 0.0).astype(BF16)


def kernel(
    t1_hbm, t2_hbm, pl_hbm, pr_hbm, out_ref,
    t1_ref, t2_ref, pl_ref, pr_ref, t1x, spread, t2s, plt, prt, wf, yb0, yb1, acc, t1s, pieces, t2p,
    part, extra, from_z, extra_z, rows, ready, arrived,
    loaded, sent, t1_got, piece_got, z_got, extra_got, row_got,
):
    i = lax.axis_index("row")
    j = lax.axis_index("col")
    x, zh, y = lax.rem(i, 4), lax.rem(i // 4, 2), i // 8
    core, zl = lax.rem(j, 2), j // 2
    other = 1 - core
    twin = 2 * zl + other
    zpeers = [(lax.rem(zl + k, 4), 2 * lax.rem(zl + k, 4) + core) for k in range(1, 4)]

    def row_of(dz, dy, dx):
        return (lax.rem(y + dy, 4) * 2 + lax.rem(zh + dz, 2)) * 4 + lax.rem(x + dx, 4)

    loads = []
    for k, (src, dst) in enumerate(
        ((t2_hbm, t2_ref), (t1_hbm, t1_ref), (pl_hbm, pl_ref), (pr_hbm, pr_ref))
    ):
        loads.append(pltpu.make_async_copy(src, dst, loaded.at[k]))
        loads[-1].start()
    barrier = pltpu.get_barrier_semaphore()
    near = [row_of(0, 0, 1), row_of(0, 0, 3), row_of(0, 1, 0), row_of(0, 3, 0), row_of(1, 0, 0)]
    for peer in near:
        pl.semaphore_signal(barrier, inc=1, device_id={"row": peer}, device_id_type=MESH)
    for col in [twin] + [col for _, col in zpeers]:
        pl.semaphore_signal(barrier, inc=1, device_id={"col": col}, device_id_type=MESH)

    spread[...] = jnp.zeros_like(spread)
    loads[0].wait()
    t2 = t2_ref[...].astype(jnp.float32)
    for c in range(2):
        for z in range(4):
            at = 6 * CHI * (2 * z + c)
            spread[c, ROWS * z : ROWS * z + ROWS, 0 : 5 * CHI] = t2[:, at : at + 5 * CHI]
            slot = CHI * SLOTS[z]
            spread[c, 4 * ROWS : 5 * ROWS, slot : slot + CHI] = t2[:, at + 5 * CHI : at + 6 * CHI]
    t2s[...] = spread[...].astype(BF16)
    pieces[i, core] = t2s[core]
    loads[1].wait()

    pl.semaphore_wait(barrier, 5 + 1 + 3)

    counts = [0] * 6

    def remote(src, dst, kind, got, where):
        return pltpu.make_async_remote_copy(
            src_ref=src, dst_ref=dst, send_sem=sent.at[kind], recv_sem=got,
            device_id=where, device_id_type=MESH,
        )

    def send(kind, src, dst, got, where):
        remote(src, dst, kind, got, where).start()
        counts[kind] += 1

    def await_copy(ref, got):
        remote(ref, ref, 0, got, {"col": twin}).wait_recv()

    def await_sent(kind, ref):
        remote(ref, ref, kind, t1_got, {"col": twin}).wait_send()

    def place(cr, dz, a, b):
        return row_of(dz, b, a) if cr == 0 else row_of(dz, a, b)

    def block(cr):
        return core if cr == 0 else other

    def pass_on(cr, dz, a, b, to_z=(), to_a=(), to_b=()):
        source, c = place(cr, dz, a, b), block(cr)
        own = cr == 0 and dz == 0 and a == 0 and b == 0
        src = t2s.at[core] if own else pieces.at[source, c]
        targets = [place(cr, 1, 0, 0) for _ in to_z]
        targets += [place(cr, 0, t, 0) for t in to_a] + [place(cr, 0, 0, t) for t in to_b]
        for target in targets:
            send(0, src, pieces.at[source, c], piece_got.at[source, c], {"row": target})

    def await_piece(cr, dz, a, b):
        source, c = place(cr, dz, a, b), block(cr)
        await_copy(pieces.at[source, c], piece_got.at[source, c])

    lane = lax.broadcasted_iota(jnp.int32, (CHI, LANES), 1)
    zero = jnp.zeros((CHI, LANES), BF16)
    swap = one_hot((192, 192), lambda r, c: (r // 8 == c % 24) & (r % 8 == c // 24))

    def weigh(ag, _):
        left = t1s[...]
        results = []
        for k in range(8):
            at = pl.multiple_of((8 * ag + k) * CHI, CHI)
            w = jnp.concatenate([plt[h, pl.ds(at, CHI), :] for h in range(2)], axis=1).astype(BF16)
            weights = jnp.concatenate(
                [jnp.where((lane >= CHI * m) & (lane < CHI * (m + 1)), w, zero) for m in range(4)], axis=0
            )
            results.append(f32dot(left, weights))
        for t in range(3):
            for s in range(3):
                at = 72 * t + 24 * s
                block = jnp.concatenate([r[at : at + 24] for r in results], axis=0).astype(BF16)
                turned = f32dot(swap, block)
                for q in range(24):
                    to = pl.multiple_of((24 * s + q) * CHI + 8 * ag, 8)
                    wf[pl.ds(to, 8), LANES * t : LANES * t + LANES] = turned[8 * q : 8 * q + 8]
        return _

    done = [0]

    def weigh_some(count):
        lax.fori_loop(done[0], done[0] + count, weigh, 0)
        done[0] += count

    send(5, t2s.at[other], pieces.at[i, core], piece_got.at[i, core], {"col": twin})
    send(1, t1_ref, t1x, t1_got, {"col": twin})
    pass_on(0, 0, 0, 0, to_z=(1,), to_a=(1, 3), to_b=(1, 3))
    await_piece(1, 0, 0, 0)
    pass_on(1, 0, 0, 0, to_z=(1,), to_a=(1, 3), to_b=(1, 3))

    place_right = one_hot((CHI, LANES), lambda r, c: (r == c % CHI) & (c < 5 * CHI))
    loads[2].wait()
    left_proj = pl_ref[...].astype(jnp.float32)
    for k in range(CHI):
        z = f32dot(left_proj[:, CHI * k : CHI * k + CHI].astype(BF16), place_right)
        for h in range(2):
            plt[h, pl.ds(k, CHI, stride=CHI), :] = z[:, 128 * h : 128 * h + 128]
    acc[...] = jnp.zeros_like(acc)
    await_copy(t1x, t1_got)
    mine, theirs = t1_ref[...].astype(jnp.float32), t1x[...].astype(jnp.float32)
    lower = jnp.where(core == 0, mine, theirs)
    upper = jnp.where(core == 0, theirs, mine)
    both = jnp.concatenate([lower, upper], axis=1)
    t1s[...] = jnp.concatenate(
        [both[:, TILE * t : TILE * t + TILE] for t in range(3)], axis=0
    ).astype(BF16)
    for t in range(3):
        t2p[LANES * t + TILE : LANES * t + LANES, :] = jnp.zeros(
            (LANES - TILE, GROUPS * LANES), BF16
        )

    def first_axis(dz):
        for cr in range(2):
            await_piece(cr, dz, 3, 0)
            pass_on(cr, dz, 3, 0, to_a=(1,) if dz == 0 else (), to_b=(1, 3))
            await_piece(cr, dz, 1, 0)
            pass_on(cr, dz, 1, 0, to_a=(3,) if dz == 1 else (), to_b=(1, 3))

    def first_axis_end(dz):
        for cr in range(2):
            await_piece(cr, dz, 2, 0)
            pass_on(cr, dz, 2, 0, to_b=(1, 3))

    def second_axis(dz, a):
        for cr in range(2):
            await_piece(cr, dz, a, 3)
            if dz == 0:
                pass_on(cr, dz, a, 3, to_b=(1,))
            await_piece(cr, dz, a, 1)
            if dz == 1:
                pass_on(cr, dz, a, 1, to_b=(3,))

    def second_axis_end(dz, a):
        for cr in range(2):
            await_piece(cr, dz, a, 2)

    def pack(g):
        w = row_window(g)
        for v in range(3):
            pick = one_hot(
                (CHI, 6 * 32),
                lambda r, c: c == (r + 3 * v) // ROWS * 32 + ROWS * g - w + (r + 3 * v) % ROWS,
            )
            for m in range(v, 12, 3):
                first = CHI * (m % 6) // ROWS
                source = pieces[first : first + 6, m // 6, w : w + 32, :].reshape(192, LANES)
                to = LANES * (m // 4) + CHI * (m % 4)
                t2p[to : to + CHI, LANES * g : LANES * g + LANES] = f32dot(pick, source).astype(BF16)

    first_axis(0)
    weigh_some(2)
    first_axis_end(0)
    weigh_some(2)
    second_axis(0, 0)
    second_axis(0, 3)
    second_axis(0, 1)
    weigh_some(2)
    for cr in range(2):
        await_piece(cr, 1, 0, 0)
        pass_on(cr, 1, 0, 0, to_a=(1, 3), to_b=(1, 3))
    second_axis(0, 2)
    first_axis(1)
    first_axis_end(1)
    for a in (0, 3, 1, 2):
        second_axis_end(0, a)
    second_axis(1, 0)
    for a in (3, 1):
        second_axis(1, a)
    loads[3].wait()
    prt[...] = lax.dot_general(
        pr_ref[...], place_right, (((0,), (0,)), ((), ())), preferred_element_type=jnp.float32
    ).astype(BF16)
    second_axis(1, 2)
    for a in (0, 3, 1, 2):
        second_axis_end(1, a)

    p = lax.rem(i, 2)

    def diag(r):
        w = prt[pl.ds(pl.multiple_of(r * CHI, CHI), CHI), :]
        parts = [
            jnp.where((lane >= CHI * e) & (lane < CHI * (e + 1)), w, zero) for e in range(5)
        ]
        return jnp.concatenate(parts + [zero[:16]], axis=0)

    size = NB * CHI

    def project(it, yb, k):
        to, parts, shift = ((0, (0, 1), 0), (96, (2,), 24))[k]
        r = lax.rem(NB * it + 24 * p + shift, CHI)
        rows_here = CHI * len(parts)
        weights = jnp.concatenate([diag(r + k) for k in range(NB)], axis=0)
        sides = []
        for k in range(NB):
            side = [yb[:, size * s + CHI * k : size * s + CHI * k + CHI, :] for s in parts]
            sides.append(jnp.concatenate(side, axis=1).reshape(GROUPS * rows_here, LANES))
        z = f32dot(jnp.concatenate(sides, axis=1), weights)
        acc[:, to : to + rows_here, :] += z.reshape(GROUPS, rows_here, LANES)

    def step(it, yb, other_yb):
        starts = [pl.multiple_of((24 * s + NB * it) * CHI, CHI) for s in (0, 2, 1)]
        w = jnp.concatenate([wf[pl.ds(at, size), :] for at in starts], axis=0).astype(BF16)
        for g in range(GROUPS):
            if other_yb is None:
                pack(g)
            elif g == 1 or g == 3:
                project(it - 1, other_yb, g // 2)
            yb[g] = f32dot(w, t2p[:, g * LANES : (g + 1) * LANES]).astype(BF16)

    def two_steps(k, _):
        step(2 * k + 1, yb1, yb0)
        step(2 * k + 2, yb0, yb1)
        return _

    last = 24 // NB - 1
    step(0, yb0, None)
    lax.fori_loop(0, (last - 1) // 2, two_steps, 0)
    step(last, yb1, yb0)
    project(last, yb1, 0)
    project(last, yb1, 1)

    mid = acc[:, 96:144, :]
    none = jnp.zeros_like(mid)
    part[:, 0:48, :] = (acc[:, 0:48, :] + jnp.where(p == 0, mid, none)).astype(BF16)
    part[:, 48:96, :] = (acc[:, 48:96, :] + jnp.where(p == 0, none, mid)).astype(BF16)
    pad = jnp.zeros((CHI, 32), jnp.float32)
    sixths = part[4].astype(jnp.float32)
    for z in range(4):
        cut = slice(CHI * SLOTS[z], CHI * SLOTS[z] + CHI)
        extra[z] = jnp.concatenate([sixths[0:48, cut], sixths[48:96, cut], pad], axis=1).astype(BF16)
    for z, col in zpeers:
        send(2, part.at[z], from_z.at[zl], z_got, {"col": col})
        send(3, extra.at[z], extra_z.at[zl], extra_got, {"col": col})
    summed = part[zl].astype(jnp.float32)
    sixth = extra[zl].astype(jnp.float32)
    await_copy(from_z.at[0:3], z_got)
    await_copy(extra_z.at[0:3], extra_got)
    for z, _ in zpeers:
        summed += from_z[z].astype(jnp.float32)
        sixth += extra_z[z].astype(jnp.float32)
    for e in range(5):
        cut = slice(CHI * e, CHI * e + CHI)
        rows[CHI * e : CHI * e + CHI] = jnp.concatenate(
            [summed[0:48, cut], summed[48:96, cut], pad], axis=1
        )
    rows[240:288] = sixth
    rows[288:304] = jnp.zeros((16, 128), jnp.float32)
    for k in range(PEERS):
        ready[k] = rows[ROWS * k : ROWS * k + 16].astype(BF16)

    for k in range(1, PEERS):
        target = lax.rem(i + k, PEERS)
        send(4, ready.at[target], arrived.at[i], row_got, {"row": target})
    arrived[i] = ready[i]
    await_copy(arrived.at[0 : PEERS - 1], row_got)
    blocks = []
    for t in range(16):
        even, odd = arrived[2 * t].astype(jnp.float32), arrived[2 * t + 1].astype(jnp.float32)
        blocks += [even[:, 0:48], even[:, 48:96] + odd[:, 0:48], odd[:, 48:96]]
    out_ref[...] = jnp.concatenate(blocks, axis=1)[0:ROWS].astype(BF16)

    assert counts == [2 * (counts[0] // 2), 1, 3, 3, PEERS - 1, 1], counts
    await_sent(0, pieces.at[0 : counts[0] // 2])
    await_sent(5, t2s.at[0])
    await_sent(1, t1x)
    await_sent(2, from_z.at[0:3])
    await_sent(3, extra_z.at[0:3])
    await_sent(4, arrived.at[0 : PEERS - 1])


def local(top_tensor, bottom_tensor, left_proj, right_proj):
    dma = pltpu.SemaphoreType.DMA
    return pl.pallas_call(
        kernel,
        out_shape=OUT,
        in_specs=[pl.BlockSpec(memory_space=pl.ANY)] * 4,
        out_specs=pl.BlockSpec(memory_space=pltpu.VMEM),
        scratch_shapes=[
            pltpu.VMEM((72, 288), BF16),
            pltpu.VMEM((ROWS, CHI * CHI), BF16),
            pltpu.VMEM((CHI, CHI * CHI), BF16),
            pltpu.VMEM((CHI, CHI * CHI), BF16),
            pltpu.VMEM((72, 288), BF16),
            pltpu.VMEM((2, 48, LANES), jnp.float32),
            pltpu.VMEM((2, 48, LANES), BF16),
            pltpu.VMEM((2, CHI * CHI, 128), jnp.float32),
            pltpu.VMEM((CHI * CHI, LANES), BF16),
            pltpu.VMEM((72 * CHI, 3 * LANES), jnp.float32),
            pltpu.VMEM((GROUPS, 3 * NB * CHI, LANES), BF16),
            pltpu.VMEM((GROUPS, 3 * NB * CHI, LANES), BF16),
            pltpu.VMEM((GROUPS, 144, LANES), jnp.float32),
            pltpu.VMEM((3 * 72, TILE), BF16),
            pltpu.VMEM((PEERS, 2, 48, LANES), BF16),
            pltpu.VMEM((3 * LANES, GROUPS * LANES), BF16),
            pltpu.VMEM((GROUPS, 96, LANES), BF16),
            pltpu.VMEM((4, CHI, 128), BF16),
            pltpu.VMEM((4, 96, LANES), BF16),
            pltpu.VMEM((4, CHI, 128), BF16),
            pltpu.VMEM((304, 128), jnp.float32),
            pltpu.VMEM((PEERS, 16, 128), BF16),
            pltpu.VMEM((PEERS, 16, 128), BF16),
            dma((4,)),
            dma((6,)),
            dma,
            dma((PEERS, 2)),
            dma,
            dma,
            dma,
        ],
        compiler_params=pltpu.CompilerParams(
            vmem_limit_bytes=60 * 1024 * 1024, collective_id=0, has_side_effects=True
        ),
    )(top_tensor, bottom_tensor, left_proj.T, right_proj.T)


def solution(mesh):
    return jax.shard_map(
        local,
        mesh=mesh,
        in_specs=(P("row", "col"), P(("col", "row"), None), P(), P()),
        out_specs=P(("col", "row"), None),
        check_vma=False,
    )
```

```python
import jax
import jax.numpy as jnp
from jax import lax
from jax.experimental import pallas as pl
from jax.experimental.pallas import tpu as pltpu
from jax.sharding import PartitionSpec as P

CHI = 48
LANES = 256
ROWS = 9
TILE = 4 * CHI
GROUPS = 5
NB = 4
OUT = pltpu.VMEM((9, 2304), jnp.bfloat16)
PEERS = 32
FAR = (3, 1, 2)
MESH = pl.DeviceIdType.MESH
BF16 = jnp.bfloat16
SLOTS = (0, 1, 3, 4)


def row_window(g):
    return min(ROWS * g // 16 * 16, 16)


def f32dot(a, b):
    return jnp.dot(a, b, preferred_element_type=jnp.float32)


def one_hot(shape, hit):
    row = lax.broadcasted_iota(jnp.int32, shape, 0)
    col = lax.broadcasted_iota(jnp.int32, shape, 1)
    return jnp.where(hit(row, col), 1.0, 0.0).astype(BF16)


def kernel(
    t1_hbm, t2_hbm, pl_hbm, pr_hbm, out_ref,
    t1_ref, t2_ref, pl_ref, pr_ref, t1x, spread, t2s, plt, prt, wf, yb0, yb1, acc, t1s, pieces, t2p,
    part, extra, from_z, extra_z, rows, ready, arrived,
    loaded, sent, t1_got, piece_got, z_got, extra_got, row_got,
):
    i = lax.axis_index("row")
    j = lax.axis_index("col")
    x, zh, y = lax.rem(i, 4), lax.rem(i // 4, 2), i // 8
    core, zl = lax.rem(j, 2), j // 2
    other = 1 - core
    twin = 2 * zl + other
    zpeers = [(lax.rem(zl + k, 4), 2 * lax.rem(zl + k, 4) + core) for k in range(1, 4)]

    def row_of(dz, dy, dx):
        return (lax.rem(y + dy, 4) * 2 + lax.rem(zh + dz, 2)) * 4 + lax.rem(x + dx, 4)

    loads = []
    for k, (src, dst) in enumerate(
        ((t2_hbm, t2_ref), (t1_hbm, t1_ref), (pl_hbm, pl_ref), (pr_hbm, pr_ref))
    ):
        loads.append(pltpu.make_async_copy(src, dst, loaded.at[k]))
        loads[-1].start()
    barrier = pltpu.get_barrier_semaphore()
    near = [row_of(0, 0, k) for k in FAR] + [row_of(0, k, 0) for k in FAR] + [row_of(1, 0, 0)]
    for peer in near:
        pl.semaphore_signal(barrier, inc=1, device_id={"row": peer}, device_id_type=MESH)
    for col in [twin] + [col for _, col in zpeers]:
        pl.semaphore_signal(barrier, inc=1, device_id={"col": col}, device_id_type=MESH)

    spread[...] = jnp.zeros_like(spread)
    loads[0].wait()
    t2 = t2_ref[...].astype(jnp.float32)
    for c in range(2):
        for z in range(4):
            at = 6 * CHI * (2 * z + c)
            spread[c, ROWS * z : ROWS * z + ROWS, 0 : 5 * CHI] = t2[:, at : at + 5 * CHI]
            slot = CHI * SLOTS[z]
            spread[c, 4 * ROWS : 5 * ROWS, slot : slot + CHI] = t2[:, at + 5 * CHI : at + 6 * CHI]
    t2s[...] = spread[...].astype(BF16)
    pieces[i, core] = t2s[core]
    loads[1].wait()

    pl.semaphore_wait(barrier, 7 + 1 + 3)

    counts = [0] * 6

    def remote(src, dst, kind, got, where):
        return pltpu.make_async_remote_copy(
            src_ref=src, dst_ref=dst, send_sem=sent.at[kind], recv_sem=got,
            device_id=where, device_id_type=MESH,
        )

    def send(kind, src, dst, got, where):
        remote(src, dst, kind, got, where).start()
        counts[kind] += 1

    def await_copy(ref, got):
        remote(ref, ref, 0, got, {"col": twin}).wait_recv()

    def await_sent(kind, ref):
        remote(ref, ref, kind, t1_got, {"col": twin}).wait_send()

    def place(cr, dz, a, b):
        return row_of(dz, b, a) if cr == 0 else row_of(dz, a, b)

    def block(cr):
        return core if cr == 0 else other

    def pass_on(cr, dz, a, b, to_z=(), to_a=(), to_b=()):
        source, c = place(cr, dz, a, b), block(cr)
        own = cr == 0 and dz == 0 and a == 0 and b == 0
        src = t2s.at[core] if own else pieces.at[source, c]
        targets = [place(cr, 1, 0, 0) for _ in to_z]
        targets += [place(cr, 0, t, 0) for t in to_a] + [place(cr, 0, 0, t) for t in to_b]
        for target in targets:
            send(0, src, pieces.at[source, c], piece_got.at[source, c], {"row": target})

    def await_piece(cr, dz, a, b):
        source, c = place(cr, dz, a, b), block(cr)
        await_copy(pieces.at[source, c], piece_got.at[source, c])

    lane = lax.broadcasted_iota(jnp.int32, (CHI, LANES), 1)
    zero = jnp.zeros((CHI, LANES), BF16)
    swap = one_hot((192, 192), lambda r, c: (r // 8 == c % 24) & (r % 8 == c // 24))

    def weigh(ag, _):
        left = t1s[...]
        results = []
        for k in range(8):
            at = pl.multiple_of((8 * ag + k) * CHI, CHI)
            w = jnp.concatenate([plt[h, pl.ds(at, CHI), :] for h in range(2)], axis=1).astype(BF16)
            weights = jnp.concatenate(
                [jnp.where((lane >= CHI * m) & (lane < CHI * (m + 1)), w, zero) for m in range(4)], axis=0
            )
            results.append(f32dot(left, weights))
        for t in range(3):
            for s in range(3):
                at = 72 * t + 24 * s
                block = jnp.concatenate([r[at : at + 24] for r in results], axis=0).astype(BF16)
                turned = f32dot(swap, block)
                for q in range(24):
                    to = pl.multiple_of((24 * s + q) * CHI + 8 * ag, 8)
                    wf[pl.ds(to, 8), LANES * t : LANES * t + LANES] = turned[8 * q : 8 * q + 8]
        return _

    done = [0]

    def weigh_some(count):
        lax.fori_loop(done[0], done[0] + count, weigh, 0)
        done[0] += count

    send(5, t2s.at[other], pieces.at[i, core], piece_got.at[i, core], {"col": twin})
    send(1, t1_ref, t1x, t1_got, {"col": twin})
    pass_on(0, 0, 0, 0, to_z=(1,), to_a=FAR, to_b=FAR)
    await_piece(1, 0, 0, 0)
    pass_on(1, 0, 0, 0, to_z=(1,), to_a=FAR, to_b=FAR)

    place_right = one_hot((CHI, LANES), lambda r, c: (r == c % CHI) & (c < 5 * CHI))
    loads[2].wait()
    left_proj = pl_ref[...].astype(jnp.float32)
    for k in range(CHI):
        z = f32dot(left_proj[:, CHI * k : CHI * k + CHI].astype(BF16), place_right)
        for h in range(2):
            plt[h, pl.ds(k, CHI, stride=CHI), :] = z[:, 128 * h : 128 * h + 128]
    acc[...] = jnp.zeros_like(acc)
    await_copy(t1x, t1_got)
    mine, theirs = t1_ref[...].astype(jnp.float32), t1x[...].astype(jnp.float32)
    lower = jnp.where(core == 0, mine, theirs)
    upper = jnp.where(core == 0, theirs, mine)
    both = jnp.concatenate([lower, upper], axis=1)
    t1s[...] = jnp.concatenate(
        [both[:, TILE * t : TILE * t + TILE] for t in range(3)], axis=0
    ).astype(BF16)
    for t in range(3):
        t2p[LANES * t + TILE : LANES * t + LANES, :] = jnp.zeros(
            (LANES - TILE, GROUPS * LANES), BF16
        )

    def relay(dz):
        for cr in range(2):
            for a in FAR:
                await_piece(cr, dz, a, 0)
                pass_on(cr, dz, a, 0, to_b=FAR)

    def collect(dz):
        for cr in range(2):
            for a in (0, *FAR):
                for b in FAR:
                    await_piece(cr, dz, a, b)

    def pack(g):
        w = row_window(g)
        for v in range(3):
            pick = one_hot(
                (CHI, 6 * 32),
                lambda r, c: c == (r + 3 * v) // ROWS * 32 + ROWS * g - w + (r + 3 * v) % ROWS,
            )
            for m in range(v, 12, 3):
                first = CHI * (m % 6) // ROWS
                source = pieces[first : first + 6, m // 6, w : w + 32, :].reshape(192, LANES)
                to = LANES * (m // 4) + CHI * (m % 4)
                t2p[to : to + CHI, LANES * g : LANES * g + LANES] = f32dot(pick, source).astype(BF16)

    weigh_some(2)
    relay(0)
    weigh_some(2)
    for cr in range(2):
        await_piece(cr, 1, 0, 0)
        pass_on(cr, 1, 0, 0, to_a=FAR, to_b=FAR)
    weigh_some(2)
    relay(1)
    loads[3].wait()
    prt[...] = lax.dot_general(
        pr_ref[...], place_right, (((0,), (0,)), ((), ())), preferred_element_type=jnp.float32
    ).astype(BF16)
    collect(0)
    collect(1)

    p = lax.rem(i, 2)

    def diag(r):
        w = prt[pl.ds(pl.multiple_of(r * CHI, CHI), CHI), :]
        parts = [
            jnp.where((lane >= CHI * e) & (lane < CHI * (e + 1)), w, zero) for e in range(5)
        ]
        return jnp.concatenate(parts + [zero[:16]], axis=0)

    size = NB * CHI

    def project(it, yb, k):
        to, parts, shift = ((0, (0, 1), 0), (96, (2,), 24))[k]
        r = lax.rem(NB * it + 24 * p + shift, CHI)
        rows_here = CHI * len(parts)
        weights = jnp.concatenate([diag(r + k) for k in range(NB)], axis=0)
        sides = []
        for k in range(NB):
            side = [yb[:, size * s + CHI * k : size * s + CHI * k + CHI, :] for s in parts]
            sides.append(jnp.concatenate(side, axis=1).reshape(GROUPS * rows_here, LANES))
        z = f32dot(jnp.concatenate(sides, axis=1), weights)
        acc[:, to : to + rows_here, :] += z.reshape(GROUPS, rows_here, LANES)

    def step(it, yb, other_yb):
        starts = [pl.multiple_of((24 * s + NB * it) * CHI, CHI) for s in (0, 2, 1)]
        w = jnp.concatenate([wf[pl.ds(at, size), :] for at in starts], axis=0).astype(BF16)
        for g in range(GROUPS):
            if other_yb is None:
                pack(g)
            elif g == 1 or g == 3:
                project(it - 1, other_yb, g // 2)
            yb[g] = f32dot(w, t2p[:, g * LANES : (g + 1) * LANES]).astype(BF16)

    def two_steps(k, _):
        step(2 * k + 1, yb1, yb0)
        step(2 * k + 2, yb0, yb1)
        return _

    last = 24 // NB - 1
    step(0, yb0, None)
    lax.fori_loop(0, (last - 1) // 2, two_steps, 0)
    step(last, yb1, yb0)
    project(last, yb1, 0)
    project(last, yb1, 1)

    mid = acc[:, 96:144, :]
    none = jnp.zeros_like(mid)
    part[:, 0:48, :] = (acc[:, 0:48, :] + jnp.where(p == 0, mid, none)).astype(BF16)
    part[:, 48:96, :] = (acc[:, 48:96, :] + jnp.where(p == 0, none, mid)).astype(BF16)
    pad = jnp.zeros((CHI, 32), jnp.float32)
    sixths = part[4].astype(jnp.float32)
    for z in range(4):
        cut = slice(CHI * SLOTS[z], CHI * SLOTS[z] + CHI)
        extra[z] = jnp.concatenate([sixths[0:48, cut], sixths[48:96, cut], pad], axis=1).astype(BF16)
    for z, col in zpeers:
        send(2, part.at[z], from_z.at[zl], z_got, {"col": col})
        send(3, extra.at[z], extra_z.at[zl], extra_got, {"col": col})
    summed = part[zl].astype(jnp.float32)
    sixth = extra[zl].astype(jnp.float32)
    await_copy(from_z.at[0:3], z_got)
    await_copy(extra_z.at[0:3], extra_got)
    for z, _ in zpeers:
        summed += from_z[z].astype(jnp.float32)
        sixth += extra_z[z].astype(jnp.float32)
    for e in range(5):
        cut = slice(CHI * e, CHI * e + CHI)
        rows[CHI * e : CHI * e + CHI] = jnp.concatenate(
            [summed[0:48, cut], summed[48:96, cut], pad], axis=1
        )
    rows[240:288] = sixth
    rows[288:304] = jnp.zeros((16, 128), jnp.float32)
    for k in range(PEERS):
        ready[k] = rows[ROWS * k : ROWS * k + 16].astype(BF16)

    for k in range(1, PEERS):
        target = lax.rem(i + k, PEERS)
        send(4, ready.at[target], arrived.at[i], row_got, {"row": target})
    arrived[i] = ready[i]
    await_copy(arrived.at[0 : PEERS - 1], row_got)
    blocks = []
    for t in range(16):
        even, odd = arrived[2 * t].astype(jnp.float32), arrived[2 * t + 1].astype(jnp.float32)
        blocks += [even[:, 0:48], even[:, 48:96] + odd[:, 0:48], odd[:, 48:96]]
    out_ref[...] = jnp.concatenate(blocks, axis=1)[0:ROWS].astype(BF16)

    assert counts == [2 * (counts[0] // 2), 1, 3, 3, PEERS - 1, 1], counts
    await_sent(0, pieces.at[0 : counts[0] // 2])
    await_sent(5, t2s.at[0])
    await_sent(1, t1x)
    await_sent(2, from_z.at[0:3])
    await_sent(3, extra_z.at[0:3])
    await_sent(4, arrived.at[0 : PEERS - 1])


def local(top_tensor, bottom_tensor, left_proj, right_proj):
    dma = pltpu.SemaphoreType.DMA
    return pl.pallas_call(
        kernel,
        out_shape=OUT,
        in_specs=[pl.BlockSpec(memory_space=pl.ANY)] * 4,
        out_specs=pl.BlockSpec(memory_space=pltpu.VMEM),
        scratch_shapes=[
            pltpu.VMEM((72, 288), BF16),
            pltpu.VMEM((ROWS, CHI * CHI), BF16),
            pltpu.VMEM((CHI, CHI * CHI), BF16),
            pltpu.VMEM((CHI, CHI * CHI), BF16),
            pltpu.VMEM((72, 288), BF16),
            pltpu.VMEM((2, 48, LANES), jnp.float32),
            pltpu.VMEM((2, 48, LANES), BF16),
            pltpu.VMEM((2, CHI * CHI, 128), jnp.float32),
            pltpu.VMEM((CHI * CHI, LANES), BF16),
            pltpu.VMEM((72 * CHI, 3 * LANES), jnp.float32),
            pltpu.VMEM((GROUPS, 3 * NB * CHI, LANES), BF16),
            pltpu.VMEM((GROUPS, 3 * NB * CHI, LANES), BF16),
            pltpu.VMEM((GROUPS, 144, LANES), jnp.float32),
            pltpu.VMEM((3 * 72, TILE), BF16),
            pltpu.VMEM((PEERS, 2, 48, LANES), BF16),
            pltpu.VMEM((3 * LANES, GROUPS * LANES), BF16),
            pltpu.VMEM((GROUPS, 96, LANES), BF16),
            pltpu.VMEM((4, CHI, 128), BF16),
            pltpu.VMEM((4, 96, LANES), BF16),
            pltpu.VMEM((4, CHI, 128), BF16),
            pltpu.VMEM((304, 128), jnp.float32),
            pltpu.VMEM((PEERS, 16, 128), BF16),
            pltpu.VMEM((PEERS, 16, 128), BF16),
            dma((4,)),
            dma((6,)),
            dma,
            dma((PEERS, 2)),
            dma,
            dma,
            dma,
        ],
        compiler_params=pltpu.CompilerParams(
            vmem_limit_bytes=60 * 1024 * 1024, collective_id=0, has_side_effects=True
        ),
    )(top_tensor, bottom_tensor, left_proj.T, right_proj.T)


def solution(mesh):
    return jax.shard_map(
        local,
        mesh=mesh,
        in_specs=(P("row", "col"), P(("col", "row"), None), P(), P()),
        out_specs=P(("col", "row"), None),
        check_vma=False,
    )
```

```python
import jax
import jax.numpy as jnp
from jax import lax
from jax.experimental import pallas as pl
from jax.experimental.pallas import tpu as pltpu
from jax.sharding import PartitionSpec as P

CHI = 48
LANES = 256
ROWS = 9
TILE = 4 * CHI
GROUPS = 5
SLOTS_HERE = 12
STEP = SLOTS_HERE * CHI
OUT = pltpu.VMEM((9, 2304), jnp.bfloat16)
PEERS = 32
FAR = (3, 1, 2)
MESH = pl.DeviceIdType.MESH
BF16 = jnp.bfloat16
SLOTS = (0, 1, 3, 4)


def row_window(g):
    return min(ROWS * g // 16 * 16, 16)


def f32dot(a, b):
    return jnp.dot(a, b, preferred_element_type=jnp.float32)


def one_hot(shape, hit):
    row = lax.broadcasted_iota(jnp.int32, shape, 0)
    col = lax.broadcasted_iota(jnp.int32, shape, 1)
    return jnp.where(hit(row, col), 1.0, 0.0).astype(BF16)


def kernel(
    t1_hbm, t2_hbm, pl_hbm, pr_hbm, out_ref,
    t1_ref, t2_ref, pl_ref, pr_ref, t1x, spread, t2s, plt, prt, wf, yb0, yb1, acc_half, acc_whole, t1s, pieces, t2p,
    part, from_z, rows, ready, arrived,
    loaded, sent, t1_got, piece_got, z_got, row_got,
):
    i = lax.axis_index("row")
    j = lax.axis_index("col")
    x, zh, y = lax.rem(i, 4), lax.rem(i // 4, 2), i // 8
    core, zl = lax.rem(j, 2), j // 2
    other = 1 - core
    twin = 2 * zl + other
    zpeers = [(lax.rem(zl + k, 4), 2 * lax.rem(zl + k, 4) + core) for k in range(1, 4)]

    def row_of(dz, dy, dx):
        return (lax.rem(y + dy, 4) * 2 + lax.rem(zh + dz, 2)) * 4 + lax.rem(x + dx, 4)

    loads = []
    for k, (src, dst) in enumerate(
        ((t2_hbm, t2_ref), (t1_hbm, t1_ref), (pl_hbm, pl_ref), (pr_hbm, pr_ref))
    ):
        loads.append(pltpu.make_async_copy(src, dst, loaded.at[k]))
        loads[-1].start()
    barrier = pltpu.get_barrier_semaphore()
    near = [row_of(0, 0, k) for k in FAR] + [row_of(0, k, 0) for k in FAR] + [row_of(1, 0, 0)]
    for peer in near:
        pl.semaphore_signal(barrier, inc=1, device_id={"row": peer}, device_id_type=MESH)
    for col in [twin] + [col for _, col in zpeers]:
        pl.semaphore_signal(barrier, inc=1, device_id={"col": col}, device_id_type=MESH)

    spread[...] = jnp.zeros_like(spread)
    loads[0].wait()
    t2 = t2_ref[...].astype(jnp.float32)
    for c in range(2):
        for z in range(4):
            at = 6 * CHI * (2 * z + c)
            spread[c, ROWS * z : ROWS * z + ROWS, 0 : 5 * CHI] = t2[:, at : at + 5 * CHI]
            slot = CHI * SLOTS[z]
            spread[c, 4 * ROWS : 5 * ROWS, slot : slot + CHI] = t2[:, at + 5 * CHI : at + 6 * CHI]
    t2s[...] = spread[...].astype(BF16)
    pieces[i, core] = t2s[core]
    loads[1].wait()

    pl.semaphore_wait(barrier, 7 + 1 + 3)

    counts = [0] * 6

    def remote(src, dst, kind, got, where):
        return pltpu.make_async_remote_copy(
            src_ref=src, dst_ref=dst, send_sem=sent.at[kind], recv_sem=got,
            device_id=where, device_id_type=MESH,
        )

    def send(kind, src, dst, got, where):
        remote(src, dst, kind, got, where).start()
        counts[kind] += 1

    def await_copy(ref, got):
        remote(ref, ref, 0, got, {"col": twin}).wait_recv()

    def await_sent(kind, ref):
        remote(ref, ref, kind, t1_got, {"col": twin}).wait_send()

    def place(cr, dz, a, b):
        return row_of(dz, b, a) if cr == 0 else row_of(dz, a, b)

    def block(cr):
        return core if cr == 0 else other

    def pass_on(cr, dz, a, b, to_z=(), to_a=(), to_b=()):
        source, c = place(cr, dz, a, b), block(cr)
        own = cr == 0 and dz == 0 and a == 0 and b == 0
        src = t2s.at[core] if own else pieces.at[source, c]
        targets = [place(cr, 1, 0, 0) for _ in to_z]
        targets += [place(cr, 0, t, 0) for t in to_a] + [place(cr, 0, 0, t) for t in to_b]
        for target in targets:
            send(0, src, pieces.at[source, c], piece_got.at[source, c], {"row": target})

    def await_piece(cr, dz, a, b):
        source, c = place(cr, dz, a, b), block(cr)
        await_copy(pieces.at[source, c], piece_got.at[source, c])

    lane = lax.broadcasted_iota(jnp.int32, (CHI, LANES), 1)
    zero = jnp.zeros((CHI, LANES), BF16)
    swap = one_hot((192, 192), lambda r, c: (r // 8 == c % 24) & (r % 8 == c // 24))

    def weigh(ag, _):
        left = t1s[...]
        results = []
        for k in range(8):
            at = pl.multiple_of((8 * ag + k) * CHI, CHI)
            w = jnp.concatenate([plt[h, pl.ds(at, CHI), :] for h in range(2)], axis=1).astype(BF16)
            weights = jnp.concatenate(
                [jnp.where((lane >= CHI * m) & (lane < CHI * (m + 1)), w, zero) for m in range(4)], axis=0
            )
            results.append(f32dot(left, weights))
        for t in range(3):
            for s in range(3):
                at = 72 * t + 24 * s
                block = jnp.concatenate([r[at : at + 24] for r in results], axis=0).astype(BF16)
                turned = f32dot(swap, block)
                for q in range(24):
                    to = pl.multiple_of((24 * s + q) * CHI + 8 * ag, 8)
                    wf[pl.ds(to, 8), LANES * t : LANES * t + LANES] = turned[8 * q : 8 * q + 8]
        return _

    done = [0]

    def weigh_some(count):
        lax.fori_loop(done[0], done[0] + count, weigh, 0)
        done[0] += count

    send(5, t2s.at[other], pieces.at[i, core], piece_got.at[i, core], {"col": twin})
    send(1, t1_ref, t1x, t1_got, {"col": twin})
    pass_on(0, 0, 0, 0, to_z=(1,), to_a=FAR, to_b=FAR)
    await_piece(1, 0, 0, 0)
    pass_on(1, 0, 0, 0, to_z=(1,), to_a=FAR, to_b=FAR)

    place_right = one_hot((CHI, LANES), lambda r, c: (r == c % CHI) & (c < 5 * CHI))
    loads[2].wait()
    left_proj = pl_ref[...].astype(jnp.float32)
    for k in range(CHI):
        z = f32dot(left_proj[:, CHI * k : CHI * k + CHI].astype(BF16), place_right)
        for h in range(2):
            plt[h, pl.ds(k, CHI, stride=CHI), :] = z[:, 128 * h : 128 * h + 128]
    acc_half[...] = jnp.zeros_like(acc_half)
    acc_whole[...] = jnp.zeros_like(acc_whole)
    await_copy(t1x, t1_got)
    mine, theirs = t1_ref[...].astype(jnp.float32), t1x[...].astype(jnp.float32)
    lower = jnp.where(core == 0, mine, theirs)
    upper = jnp.where(core == 0, theirs, mine)
    both = jnp.concatenate([lower, upper], axis=1)
    t1s[...] = jnp.concatenate(
        [both[:, TILE * t : TILE * t + TILE] for t in range(3)], axis=0
    ).astype(BF16)
    for t in range(3):
        t2p[LANES * t + TILE : LANES * t + LANES, :] = jnp.zeros(
            (LANES - TILE, GROUPS * LANES), BF16
        )

    def relay(dz):
        for cr in range(2):
            for a in FAR:
                await_piece(cr, dz, a, 0)
                pass_on(cr, dz, a, 0, to_b=FAR)

    def collect(dz):
        for cr in range(2):
            for a in (0, *FAR):
                for b in FAR:
                    await_piece(cr, dz, a, b)

    def pack(g):
        w = row_window(g)
        for v in range(3):
            pick = one_hot(
                (CHI, 6 * 32),
                lambda r, c: c == (r + 3 * v) // ROWS * 32 + ROWS * g - w + (r + 3 * v) % ROWS,
            )
            for m in range(v, 12, 3):
                first = CHI * (m % 6) // ROWS
                source = pieces[first : first + 6, m // 6, w : w + 32, :].reshape(192, LANES)
                to = LANES * (m // 4) + CHI * (m % 4)
                t2p[to : to + CHI, LANES * g : LANES * g + LANES] = f32dot(pick, source).astype(BF16)

    weigh_some(2)
    relay(0)
    weigh_some(2)
    for cr in range(2):
        await_piece(cr, 1, 0, 0)
        pass_on(cr, 1, 0, 0, to_a=FAR, to_b=FAR)
    weigh_some(2)
    relay(1)
    loads[3].wait()
    prt[...] = lax.dot_general(
        pr_ref[...], place_right, (((0,), (0,)), ((), ())), preferred_element_type=jnp.float32
    ).astype(BF16)
    collect(0)
    collect(1)

    p = lax.rem(i, 2)

    def diag(r):
        w = prt[pl.ds(pl.multiple_of(r * CHI, CHI), CHI), :]
        parts = [
            jnp.where((lane >= CHI * e) & (lane < CHI * (e + 1)), w, zero) for e in range(5)
        ]
        return jnp.concatenate(parts + [zero[:16]], axis=0)

    base = (48 * (1 - p), 24 * p)

    def project(slot, yb, total):
        r = lax.rem(24 * p + slot, CHI)
        for k in range(0, SLOTS_HERE, 4):
            weights = jnp.concatenate([diag(r + k + q) for q in range(4)], axis=0)
            left = [
                yb[:, CHI * (k + q) : CHI * (k + q + 1), :].reshape(GROUPS * CHI, LANES)
                for q in range(4)
            ]
            z = f32dot(jnp.concatenate(left, axis=1), weights)
            total[...] += z.reshape(GROUPS, CHI, LANES)

    def multiply(slot, yb, before=None):
        w = wf[pl.ds(pl.multiple_of(slot * CHI, CHI), STEP), :].astype(BF16)
        for g in range(GROUPS):
            if before is None:
                pack(g)
            elif g == 1:
                project(*before)
            yb[g] = f32dot(w, t2p[:, g * LANES : (g + 1) * LANES]).astype(BF16)

    gap = jnp.zeros((16, 16), jnp.float32)
    wide_gap = jnp.zeros((16, 64), jnp.float32)

    def send_part(u, total):
        for z in range(4):
            part[u, z, 0:48, :] = total[z].astype(BF16)
            at = CHI * SLOTS[z]
            sixth = total[4][:, at : at + CHI]
            parts = []
            for q in range(3):
                parts += [sixth[16 * q : 16 * q + 16], gap]
            part[u, z, 48:64, :] = jnp.concatenate(parts + [wide_gap], axis=1).astype(BF16)
        for z, col in zpeers:
            send(2 + u, part.at[u, z], from_z.at[u, zl], z_got.at[u], {"col": col})

    jobs = [(base[0] + SLOTS_HERE * k, acc_half) for k in range(2)]
    jobs += [(base[1] + SLOTS_HERE * k, acc_whole) for k in range(4)]
    before = None
    for k, (slot, total) in enumerate(jobs):
        yb = (yb0, yb1)[k % 2]
        multiply(slot, yb, before)
        before = (slot, yb, total)
        if k == 2:
            send_part(0, acc_half)
    project(*before)
    send_part(1, acc_whole)

    summed = []
    for u in range(2):
        await_copy(from_z.at[u, 0:3], z_got.at[u])
        value = part[u, zl].astype(jnp.float32)
        for z, _ in zpeers:
            value += from_z[u, z].astype(jnp.float32)
        summed.append(value)
    first = jnp.where(p == 0, summed[1], summed[0])
    second = jnp.where(p == 0, summed[0], summed[1])
    pad = jnp.zeros((CHI, 32), jnp.float32)
    for e in range(5):
        cut = slice(CHI * e, CHI * e + CHI)
        rows[CHI * e : CHI * e + CHI] = jnp.concatenate(
            [first[0:48, cut], second[0:48, cut], pad], axis=1
        )
    for q in range(3):
        cut = slice(64 * q, 64 * q + CHI)
        rows[240 + 16 * q : 256 + 16 * q] = jnp.concatenate(
            [first[48:64, cut], second[48:64, cut], pad[0:16]], axis=1
        )
    rows[288:304] = jnp.zeros((16, 128), jnp.float32)
    for k in range(PEERS):
        ready[k] = rows[ROWS * k : ROWS * k + 16].astype(BF16)

    for k in range(1, PEERS):
        target = lax.rem(i + k, PEERS)
        send(4, ready.at[target], arrived.at[i], row_got, {"row": target})
    arrived[i] = ready[i]
    await_copy(arrived.at[0 : PEERS - 1], row_got)
    blocks = []
    for t in range(16):
        even, odd = arrived[2 * t].astype(jnp.float32), arrived[2 * t + 1].astype(jnp.float32)
        blocks += [even[:, 0:48], even[:, 48:96] + odd[:, 0:48], odd[:, 48:96]]
    out_ref[...] = jnp.concatenate(blocks, axis=1)[0:ROWS].astype(BF16)

    assert counts == [2 * (counts[0] // 2), 1, 3, 3, PEERS - 1, 1], counts
    await_sent(0, pieces.at[0 : counts[0] // 2])
    await_sent(5, t2s.at[0])
    await_sent(1, t1x)
    await_sent(2, from_z.at[0, 0:3])
    await_sent(3, from_z.at[1, 0:3])
    await_sent(4, arrived.at[0 : PEERS - 1])


def local(top_tensor, bottom_tensor, left_proj, right_proj):
    dma = pltpu.SemaphoreType.DMA
    return pl.pallas_call(
        kernel,
        out_shape=OUT,
        in_specs=[pl.BlockSpec(memory_space=pl.ANY)] * 4,
        out_specs=pl.BlockSpec(memory_space=pltpu.VMEM),
        scratch_shapes=[
            pltpu.VMEM((72, 288), BF16),
            pltpu.VMEM((ROWS, CHI * CHI), BF16),
            pltpu.VMEM((CHI, CHI * CHI), BF16),
            pltpu.VMEM((CHI, CHI * CHI), BF16),
            pltpu.VMEM((72, 288), BF16),
            pltpu.VMEM((2, 48, LANES), jnp.float32),
            pltpu.VMEM((2, 48, LANES), BF16),
            pltpu.VMEM((2, CHI * CHI, 128), jnp.float32),
            pltpu.VMEM((CHI * CHI, LANES), BF16),
            pltpu.VMEM((72 * CHI, 3 * LANES), jnp.float32),
            pltpu.VMEM((GROUPS, STEP, LANES), BF16),
            pltpu.VMEM((GROUPS, STEP, LANES), BF16),
            pltpu.VMEM((GROUPS, CHI, LANES), jnp.float32),
            pltpu.VMEM((GROUPS, CHI, LANES), jnp.float32),
            pltpu.VMEM((3 * 72, TILE), BF16),
            pltpu.VMEM((PEERS, 2, 48, LANES), BF16),
            pltpu.VMEM((3 * LANES, GROUPS * LANES), BF16),
            pltpu.VMEM((2, 4, 64, LANES), BF16),
            pltpu.VMEM((2, 4, 64, LANES), BF16),
            pltpu.VMEM((304, 128), jnp.float32),
            pltpu.VMEM((PEERS, 16, 128), BF16),
            pltpu.VMEM((PEERS, 16, 128), BF16),
            dma((4,)),
            dma((6,)),
            dma,
            dma((PEERS, 2)),
            dma((2,)),
            dma,
        ],
        compiler_params=pltpu.CompilerParams(
            vmem_limit_bytes=60 * 1024 * 1024, collective_id=0, has_side_effects=True
        ),
    )(top_tensor, bottom_tensor, left_proj.T, right_proj.T)


def solution(mesh):
    return jax.shard_map(
        local,
        mesh=mesh,
        in_specs=(P("row", "col"), P(("col", "row"), None), P(), P()),
        out_specs=P(("col", "row"), None),
        check_vma=False,
    )
```

```python
import jax
import jax.numpy as jnp
from jax import lax
from jax.experimental import pallas as pl
from jax.experimental.pallas import tpu as pltpu
from jax.sharding import PartitionSpec as P

CHI = 48
LANES = 256
ROWS = 9
TILE = 4 * CHI
GROUPS = 5
SLOTS_HERE = 12
STEP = SLOTS_HERE * CHI
OUT = pltpu.VMEM((9, 2304), jnp.bfloat16)
PEERS = 32
FAR = (3, 1, 2)
NEXT = (3, 1)
MESH = pl.DeviceIdType.MESH
BF16 = jnp.bfloat16
SLOTS = (0, 1, 3, 4)


STARTS = ((0, 9, 0), (16, 9, 0), (32, 9, 0), (9, 7, 9), (27, 5, 9))


def row_window(g):
    return ((0, 16), (16, 16), (32, 16), (0, 32), (16, 32))[g]


def f32dot(a, b):
    return jnp.dot(a, b, preferred_element_type=jnp.float32)


def one_hot(shape, hit):
    row = lax.broadcasted_iota(jnp.int32, shape, 0)
    col = lax.broadcasted_iota(jnp.int32, shape, 1)
    return jnp.where(hit(row, col), 1.0, 0.0).astype(BF16)


def kernel(
    t1_hbm, t2_hbm, pl_hbm, pr_hbm, out_ref,
    t1_ref, t2_ref, pl_ref, pr_ref, t1x, spread, t2s, plt, prt, wf, yb0, yb1, acc_half, acc_whole, t1s, pieces, t2p,
    part, from_z, turn, summed, ready, arrived,
    loaded, sent, t1_got, piece_got, z_got, row_got,
):
    i = lax.axis_index("row")
    j = lax.axis_index("col")
    x, zh, y = lax.rem(i, 4), lax.rem(i // 4, 2), i // 8
    core, zl = lax.rem(j, 2), j // 2
    other = 1 - core
    twin = 2 * zl + other
    def row_of(dz, dy, dx):
        return (lax.rem(y + dy, 4) * 2 + lax.rem(zh + dz, 2)) * 4 + lax.rem(x + dx, 4)

    ring = []
    for dz in range(2):
        for k in range(4):
            z = lax.rem(zl + k, 4)
            where = {"row": row_of(dz, 0, 0), "col": 2 * z + core}
            ring.append((z, lax.rem(zh + dz, 2), where))

    loads = []
    for k, (src, dst) in enumerate(
        ((t2_hbm, t2_ref), (t1_hbm, t1_ref), (pl_hbm, pl_ref), (pr_hbm, pr_ref))
    ):
        loads.append(pltpu.make_async_copy(src, dst, loaded.at[k]))
        loads[-1].start()
    barrier = pltpu.get_barrier_semaphore()
    near = [row_of(0, 0, k) for k in FAR] + [row_of(0, k, 0) for k in FAR]
    for peer in near:
        pl.semaphore_signal(barrier, inc=1, device_id={"row": peer}, device_id_type=MESH)
    pl.semaphore_signal(barrier, inc=1, device_id={"col": twin}, device_id_type=MESH)
    for _, _, where in ring[1:]:
        pl.semaphore_signal(barrier, inc=1, device_id=where, device_id_type=MESH)

    spread[...] = jnp.zeros_like(spread)
    loads[0].wait()
    t2 = t2_ref[...].astype(jnp.float32)
    for c in range(2):
        for z in range(4):
            at = 6 * CHI * (2 * z + c)
            slot = CHI * SLOTS[z]
            for g, left, lanes, width in ((z, at, 0, 5 * CHI), (4, at + 5 * CHI, slot, CHI)):
                row, run, skip = STARTS[g]
                value = t2[:, left : left + width]
                spread[c, row : row + run, lanes : lanes + width] = value[0:run]
                if run < ROWS:
                    to = row + run + skip
                    spread[c, to : to + ROWS - run, lanes : lanes + width] = value[run:ROWS]
    t2s[...] = spread[...].astype(BF16)
    pieces[i, core] = t2s[core]
    loads[1].wait()

    pl.semaphore_wait(barrier, 6 + 1 + 7)

    counts = [0] * 6

    def remote(src, dst, kind, got, where):
        return pltpu.make_async_remote_copy(
            src_ref=src, dst_ref=dst, send_sem=sent.at[kind], recv_sem=got,
            device_id=where, device_id_type=MESH,
        )

    def send(kind, src, dst, got, where):
        remote(src, dst, kind, got, where).start()
        counts[kind] += 1

    def await_copy(ref, got):
        remote(ref, ref, 0, got, {"col": twin}).wait_recv()

    def await_sent(kind, ref):
        remote(ref, ref, kind, t1_got, {"col": twin}).wait_send()

    def place(cr, dz, a, b):
        return row_of(dz, b, a) if cr == 0 else row_of(dz, a, b)

    def block(cr):
        return core if cr == 0 else other

    def pass_on(cr, dz, a, b, to_z=(), to_a=(), to_b=()):
        source, c = place(cr, dz, a, b), block(cr)
        own = cr == 0 and dz == 0 and a == 0 and b == 0
        src = t2s.at[core] if own else pieces.at[source, c]
        targets = [place(cr, 1, 0, 0) for _ in to_z]
        targets += [place(cr, 0, t, 0) for t in to_a] + [place(cr, 0, 0, t) for t in to_b]
        for target in targets:
            send(0, src, pieces.at[source, c], piece_got.at[source, c], {"row": target})

    def await_piece(cr, dz, a, b):
        source, c = place(cr, dz, a, b), block(cr)
        await_copy(pieces.at[source, c], piece_got.at[source, c])

    lane = lax.broadcasted_iota(jnp.int32, (CHI, LANES), 1)
    zero = jnp.zeros((CHI, LANES), BF16)
    swap = one_hot((192, 192), lambda r, c: (r // 8 == c % 24) & (r % 8 == c // 24))

    def weigh(ag, _):
        left = t1s[...]
        results = []
        for k in range(8):
            at = pl.multiple_of((8 * ag + k) * CHI, CHI)
            w = jnp.concatenate([plt[h, pl.ds(at, CHI), :] for h in range(2)], axis=1).astype(BF16)
            weights = jnp.concatenate(
                [jnp.where((lane >= CHI * m) & (lane < CHI * (m + 1)), w, zero) for m in range(4)], axis=0
            )
            results.append(f32dot(left, weights))
        for t in range(3):
            for s in range(3):
                at = 72 * t + 24 * s
                block = jnp.concatenate([r[at : at + 24] for r in results], axis=0).astype(BF16)
                turned = f32dot(swap, block)
                for q in range(24):
                    to = pl.multiple_of((24 * s + q) * CHI + 8 * ag, 8)
                    wf[pl.ds(to, 8), LANES * t : LANES * t + LANES] = turned[8 * q : 8 * q + 8]
        return _

    done = [0]

    def weigh_some(count):
        lax.fori_loop(done[0], done[0] + count, weigh, 0)
        done[0] += count

    send(5, t2s.at[other], pieces.at[i, core], piece_got.at[i, core], {"col": twin})
    send(1, t1_ref, t1x, t1_got, {"col": twin})
    pass_on(0, 0, 0, 0, to_z=(1,), to_a=FAR, to_b=NEXT)
    await_piece(1, 0, 0, 0)
    pass_on(1, 0, 0, 0, to_z=(1,), to_a=FAR, to_b=NEXT)

    place_right = one_hot((CHI, LANES), lambda r, c: (r == c % CHI) & (c < 5 * CHI))
    loads[2].wait()
    left_proj = pl_ref[...].astype(jnp.float32)
    for k in range(CHI):
        z = f32dot(left_proj[:, CHI * k : CHI * k + CHI].astype(BF16), place_right)
        for h in range(2):
            plt[h, pl.ds(k, CHI, stride=CHI), :] = z[:, 128 * h : 128 * h + 128]
    acc_half[...] = jnp.zeros_like(acc_half)
    turn[...] = jnp.zeros_like(turn)
    summed[...] = jnp.zeros_like(summed)
    acc_whole[...] = jnp.zeros_like(acc_whole)
    await_copy(t1x, t1_got)
    mine, theirs = t1_ref[...].astype(jnp.float32), t1x[...].astype(jnp.float32)
    lower = jnp.where(core == 0, mine, theirs)
    upper = jnp.where(core == 0, theirs, mine)
    both = jnp.concatenate([lower, upper], axis=1)
    t1s[...] = jnp.concatenate(
        [both[:, TILE * t : TILE * t + TILE] for t in range(3)], axis=0
    ).astype(BF16)
    for t in range(3):
        t2p[LANES * t + TILE : LANES * t + LANES, :] = jnp.zeros(
            (LANES - TILE, GROUPS * LANES), BF16
        )

    def relay(dz):
        for cr in range(2):
            for a in FAR:
                await_piece(cr, dz, a, 0)
                pass_on(cr, dz, a, 0, to_b=FAR if dz else NEXT)

    def relay_near():
        for cr in range(2):
            for a in (0, *FAR):
                await_piece(cr, 0, a, 1)
                pass_on(cr, 0, a, 1, to_b=(3,))

    def collect(dz):
        for cr in range(2):
            for a in (0, *FAR):
                for b in FAR:
                    if dz == 1 or b != 1:
                        await_piece(cr, dz, a, b)

    def pack(g):
        w, height = row_window(g)
        row, run, skip = STARTS[g]
        for v in range(3):

            def hit(r, c):
                q = (r + 3 * v) % ROWS
                return c == (r + 3 * v) // ROWS * height + row - w + q + jnp.where(q < run, 0, skip)

            pick = one_hot((CHI, 6 * height), hit)
            for m in range(v, 12, 3):
                first = CHI * (m % 6) // ROWS
                source = pieces[first : first + 6, m // 6, w : w + height, :]
                source = source.reshape(6 * height, LANES)
                to = LANES * (m // 4) + CHI * (m % 4)
                t2p[to : to + CHI, LANES * g : LANES * g + LANES] = f32dot(pick, source).astype(BF16)

    weigh_some(2)
    relay(0)
    weigh_some(1)
    for cr in range(2):
        await_piece(cr, 1, 0, 0)
        pass_on(cr, 1, 0, 0, to_a=FAR, to_b=FAR)
    relay_near()
    weigh_some(1)
    relay(1)
    weigh_some(2)
    loads[3].wait()
    prt[...] = lax.dot_general(
        pr_ref[...], place_right, (((0,), (0,)), ((), ())), preferred_element_type=jnp.float32
    ).astype(BF16)
    collect(0)
    collect(1)

    p = lax.rem(i, 2)

    def diag(r):
        w = prt[pl.ds(pl.multiple_of(r * CHI, CHI), CHI), :]
        parts = [
            jnp.where((lane >= CHI * e) & (lane < CHI * (e + 1)), w, zero) for e in range(5)
        ]
        return jnp.concatenate(parts + [zero[:16]], axis=0)

    base = (48 * (1 - p), 24 * p)

    def project(slot, yb, total):
        r = lax.rem(24 * p + slot, CHI)
        for k in range(0, SLOTS_HERE, 4):
            weights = jnp.concatenate([diag(r + k + q) for q in range(4)], axis=0)
            left = [
                yb[:, CHI * (k + q) : CHI * (k + q + 1), :].reshape(GROUPS * CHI, LANES)
                for q in range(4)
            ]
            z = f32dot(jnp.concatenate(left, axis=1), weights)
            total[...] += z.reshape(GROUPS, CHI, LANES)

    def multiply(slot, yb, before=None):
        w = wf[pl.ds(pl.multiple_of(slot * CHI, CHI), STEP), :].astype(BF16)
        for g in range(GROUPS):
            if before is None:
                pack(g)
            elif g == 1:
                project(*before)
            yb[g] = f32dot(w, t2p[:, g * LANES : (g + 1) * LANES]).astype(BF16)

    def send_part(u, total):
        for z in range(4):
            for e in range(5):
                turn[z, CHI * e : CHI * e + CHI, 0:CHI] = total[z][:, CHI * e : CHI * e + CHI]
            at = CHI * SLOTS[z]
            turn[z, 5 * CHI : 6 * CHI, 0:CHI] = total[4][:, at : at + CHI]
        for z in range(4):
            for h in range(2):
                low = [turn[z, 72 * q + 36 * h : 72 * q + 36 * h + 40, :] for q in range(4)]
                part[u, z, h] = jnp.concatenate(
                    [low[q] + pltpu.roll(low[2 + q], 64, 1) for q in range(2)], axis=0
                ).astype(BF16)
        from_z[u, 4 * zh + zl] = part[u, zl, zh]
        for z, h, where in ring[1:]:
            send(2 + u, part.at[u, z, h], from_z.at[u, 4 * zh + zl], z_got.at[u], where)

    jobs = [(base[0] + SLOTS_HERE * k, acc_half) for k in range(2)]
    jobs += [(base[1] + SLOTS_HERE * k, acc_whole) for k in range(4)]
    before = None
    for k, (slot, total) in enumerate(jobs):
        yb = (yb0, yb1)[k % 2]
        multiply(slot, yb, before)
        before = (slot, yb, total)
        if k == 2:
            send_part(0, acc_half)
    project(*before)
    send_part(1, acc_whole)

    for u in range(2):
        await_copy(from_z.at[u, 0:7], z_got.at[u])
    for h in range(2):
        half, whole = [
            sum(from_z[u, 4 * h + z].astype(jnp.float32) for z in range(4)) for u in range(2)
        ]
        summed[2 * h, 0:80, :] = jnp.where(p == 0, whole, half)
        summed[2 * h + 1, 0:80, :] = jnp.where(p == 0, half, whole)
    wide = lax.broadcasted_iota(jnp.int32, (16, 128), 1)
    for yt in range(4):
        for xt in range(4):
            at = 40 * (yt % 2) + ROWS * xt
            sides = []
            for h in range(2):
                first, second = [summed[2 * h + f, at : at + 16, :] for f in range(2)]
                if yt < 2:
                    second = pltpu.roll(second, 64, 1)
                else:
                    first = pltpu.roll(first, 64, 1)
                sides.append(jnp.where(wide < 64, first, second))
            ready[4 * yt + xt] = jnp.concatenate(sides, axis=1).astype(BF16)

    spot = 4 * y + x
    for dy in range(4):
        for dx in range(4):
            if dy or dx:
                target = 4 * lax.rem(y + dy, 4) + lax.rem(x + dx, 4)
                where = {"row": row_of(0, dy, dx)}
                send(4, ready.at[target], arrived.at[spot], row_got, where)
    arrived[spot] = ready[spot]
    await_copy(arrived.at[0:15], row_got)
    blocks = []
    for t in range(16):
        source, h = 4 * (t // 4) + 2 * (t % 2), t // 2 % 2
        even, odd = [arrived[source + k].astype(jnp.float32) for k in range(2)]
        one, two = 128 * h, 128 * h + 64
        blocks.append(even[:, one : one + CHI])
        blocks.append(even[:, two : two + CHI] + odd[:, one : one + CHI])
        blocks.append(odd[:, two : two + CHI])
    out_ref[...] = jnp.concatenate(blocks, axis=1)[0:ROWS].astype(BF16)

    assert counts == [2 * (counts[0] // 2), 1, 7, 7, 15, 1], counts
    await_sent(0, pieces.at[0 : counts[0] // 2])
    await_sent(5, t2s.at[0])
    await_sent(1, t1x)
    await_sent(2, from_z.at[0, 0:7])
    await_sent(3, from_z.at[1, 0:7])
    await_sent(4, arrived.at[0:15])


def local(top_tensor, bottom_tensor, left_proj, right_proj):
    dma = pltpu.SemaphoreType.DMA
    return pl.pallas_call(
        kernel,
        out_shape=OUT,
        in_specs=[pl.BlockSpec(memory_space=pl.ANY)] * 4,
        out_specs=pl.BlockSpec(memory_space=pltpu.VMEM),
        scratch_shapes=[
            pltpu.VMEM((72, 288), BF16),
            pltpu.VMEM((ROWS, CHI * CHI), BF16),
            pltpu.VMEM((CHI, CHI * CHI), BF16),
            pltpu.VMEM((CHI, CHI * CHI), BF16),
            pltpu.VMEM((72, 288), BF16),
            pltpu.VMEM((2, 48, LANES), jnp.float32),
            pltpu.VMEM((2, 48, LANES), BF16),
            pltpu.VMEM((2, CHI * CHI, 128), jnp.float32),
            pltpu.VMEM((CHI * CHI, LANES), BF16),
            pltpu.VMEM((72 * CHI, 3 * LANES), jnp.float32),
            pltpu.VMEM((GROUPS, STEP, LANES), BF16),
            pltpu.VMEM((GROUPS, STEP, LANES), BF16),
            pltpu.VMEM((GROUPS, CHI, LANES), jnp.float32),
            pltpu.VMEM((GROUPS, CHI, LANES), jnp.float32),
            pltpu.VMEM((3 * 72, TILE), BF16),
            pltpu.VMEM((PEERS, 2, 48, LANES), BF16),
            pltpu.VMEM((3 * LANES, GROUPS * LANES), BF16),
            pltpu.VMEM((2, 4, 2, 80, 128), BF16),
            pltpu.VMEM((2, 8, 80, 128), BF16),
            pltpu.VMEM((4, 296, 128), jnp.float32),
            pltpu.VMEM((4, 88, 128), jnp.float32),
            pltpu.VMEM((16, 16, LANES), BF16),
            pltpu.VMEM((16, 16, LANES), BF16),
            dma((4,)),
            dma((6,)),
            dma,
            dma((PEERS, 2)),
            dma((2,)),
            dma,
        ],
        compiler_params=pltpu.CompilerParams(
            vmem_limit_bytes=60 * 1024 * 1024, collective_id=0, has_side_effects=True
        ),
    )(top_tensor, bottom_tensor, left_proj.T, right_proj.T)


def solution(mesh):
    return jax.shard_map(
        local,
        mesh=mesh,
        in_specs=(P("row", "col"), P(("col", "row"), None), P(), P()),
        out_specs=P(("col", "row"), None),
        check_vma=False,
    )
```

```python
import jax
import jax.numpy as jnp
from jax import lax
from jax.experimental import pallas as pl
from jax.experimental.pallas import tpu as pltpu
from jax.sharding import PartitionSpec as P

CHI = 48
LANES = 256
ROWS = 9
TILE = 4 * CHI
GROUPS = 5
SLOTS_HERE = 12
STEP = SLOTS_HERE * CHI
OUT = pltpu.VMEM((9, 2304), jnp.bfloat16)
PEERS = 32
FAR = (3, 1, 2)
NEXT = (3, 1)
MESH = pl.DeviceIdType.MESH
BF16 = jnp.bfloat16
SLOTS = (0, 1, 3, 4)


STARTS = ((0, 9, 0), (16, 9, 0), (32, 9, 0), (9, 7, 9), (27, 5, 9))


def row_window(g):
    return ((0, 16), (16, 16), (32, 16), (0, 32), (16, 32))[g]


def f32dot(a, b):
    return jnp.dot(a, b, preferred_element_type=jnp.float32)


def one_hot(shape, hit):
    row = lax.broadcasted_iota(jnp.int32, shape, 0)
    col = lax.broadcasted_iota(jnp.int32, shape, 1)
    return jnp.where(hit(row, col), 1.0, 0.0).astype(BF16)


def kernel(
    t1_hbm, t2_hbm, pl_hbm, pr_hbm, out_ref,
    t1_ref, t2_ref, pl_ref, pr_ref, t1x, spread, t2s, plt, prt, wf, yb0, yb1, acc_half, acc_whole, t1s, pieces, t2p,
    part, from_z, turn, summed, ready, arrived,
    loaded, sent, t1_got, piece_got, z_got, row_got,
):
    i = lax.axis_index("row")
    j = lax.axis_index("col")
    x, zh, y = lax.rem(i, 4), lax.rem(i // 4, 2), i // 8
    core, zl = lax.rem(j, 2), j // 2
    other = 1 - core
    twin = 2 * zl + other
    def row_of(dz, dy, dx):
        return (lax.rem(y + dy, 4) * 2 + lax.rem(zh + dz, 2)) * 4 + lax.rem(x + dx, 4)

    ring = []
    for dz in range(2):
        for k in range(4):
            z = lax.rem(zl + k, 4)
            where = {"row": row_of(dz, 0, 0), "col": 2 * z + core}
            ring.append((z, lax.rem(zh + dz, 2), where))

    loads = []
    for k, (src, dst) in enumerate(
        ((t2_hbm, t2_ref), (t1_hbm, t1_ref), (pl_hbm, pl_ref), (pr_hbm, pr_ref))
    ):
        loads.append(pltpu.make_async_copy(src, dst, loaded.at[k]))
        loads[-1].start()
    barrier = pltpu.get_barrier_semaphore()
    near = [row_of(0, 0, k) for k in FAR] + [row_of(0, k, 0) for k in FAR]
    for peer in near:
        pl.semaphore_signal(barrier, inc=1, device_id={"row": peer}, device_id_type=MESH)
    pl.semaphore_signal(barrier, inc=1, device_id={"col": twin}, device_id_type=MESH)
    for _, _, where in ring[1:]:
        pl.semaphore_signal(barrier, inc=1, device_id=where, device_id_type=MESH)

    spread[...] = jnp.zeros_like(spread)
    loads[0].wait()
    t2 = t2_ref[...].astype(jnp.float32)
    for c in range(2):
        for z in range(4):
            at = 6 * CHI * (2 * z + c)
            slot = CHI * SLOTS[z]
            for g, left, lanes, width in ((z, at, 0, 5 * CHI), (4, at + 5 * CHI, slot, CHI)):
                row, run, skip = STARTS[g]
                value = t2[:, left : left + width]
                spread[c, row : row + run, lanes : lanes + width] = value[0:run]
                if run < ROWS:
                    to = row + run + skip
                    spread[c, to : to + ROWS - run, lanes : lanes + width] = value[run:ROWS]
    t2s[...] = spread[...].astype(BF16)
    pieces[i, core] = t2s[core]
    loads[1].wait()

    pl.semaphore_wait(barrier, 6 + 1 + 7)

    counts = [0] * 6

    def remote(src, dst, kind, got, where):
        return pltpu.make_async_remote_copy(
            src_ref=src, dst_ref=dst, send_sem=sent.at[kind], recv_sem=got,
            device_id=where, device_id_type=MESH,
        )

    def send(kind, src, dst, got, where):
        remote(src, dst, kind, got, where).start()
        counts[kind] += 1

    def await_copy(ref, got):
        remote(ref, ref, 0, got, {"col": twin}).wait_recv()

    def await_sent(kind, ref):
        remote(ref, ref, kind, t1_got, {"col": twin}).wait_send()

    def place(cr, dz, a, b):
        return row_of(dz, b, a) if cr == 0 else row_of(dz, a, b)

    def block(cr):
        return core if cr == 0 else other

    def place_got(cr, dz, a, b):
        if b == 0:
            return 16 * cr + 8 * dz + a
        if b == 1 and dz == 0:
            return 16 * cr + 4 + a
        return 16 * cr + 12 + dz

    def pass_on(cr, dz, a, b, to_z=(), to_a=(), to_b=()):
        source, c = place(cr, dz, a, b), block(cr)
        own = cr == 0 and dz == 0 and a == 0 and b == 0
        src = t2s.at[core] if own else pieces.at[source, c]
        targets = [(place(cr, 1, 0, 0), place_got(cr, 1, 0, 0)) for _ in to_z]
        targets += [(place(cr, 0, t, 0), place_got(cr, dz, (a - t) % 4, b)) for t in to_a]
        targets += [(place(cr, 0, 0, t), place_got(cr, dz, a, (b - t) % 4)) for t in to_b]
        for target, got in targets:
            send(0, src, pieces.at[source, c], piece_got.at[got], {"row": target})

    def await_piece(cr, dz, a, b):
        await_copy(pieces.at[place(cr, dz, a, b), block(cr)], piece_got.at[place_got(cr, dz, a, b)])

    lane = lax.broadcasted_iota(jnp.int32, (CHI, LANES), 1)
    zero = jnp.zeros((CHI, LANES), BF16)
    swap = one_hot((192, 192), lambda r, c: (r // 8 == c % 24) & (r % 8 == c // 24))

    def weigh(ag, _):
        left = t1s[...]
        results = []
        for k in range(8):
            at = pl.multiple_of((8 * ag + k) * CHI, CHI)
            w = jnp.concatenate([plt[h, pl.ds(at, CHI), :] for h in range(2)], axis=1).astype(BF16)
            weights = jnp.concatenate(
                [jnp.where((lane >= CHI * m) & (lane < CHI * (m + 1)), w, zero) for m in range(4)], axis=0
            )
            results.append(f32dot(left, weights))
        for t in range(3):
            for s in range(3):
                at = 72 * t + 24 * s
                block = jnp.concatenate([r[at : at + 24] for r in results], axis=0).astype(BF16)
                turned = f32dot(swap, block)
                for q in range(24):
                    to = pl.multiple_of((24 * s + q) * CHI + 8 * ag, 8)
                    wf[pl.ds(to, 8), LANES * t : LANES * t + LANES] = turned[8 * q : 8 * q + 8]
        return _

    done = [0]

    def weigh_some(count):
        lax.fori_loop(done[0], done[0] + count, weigh, 0)
        done[0] += count

    send(5, t2s.at[other], pieces.at[i, core], piece_got.at[16], {"col": twin})
    send(1, t1_ref, t1x, t1_got, {"col": twin})
    pass_on(0, 0, 0, 0, to_z=(1,), to_a=FAR, to_b=NEXT)
    await_piece(1, 0, 0, 0)
    pass_on(1, 0, 0, 0, to_z=(1,), to_a=FAR, to_b=NEXT)

    place_right = one_hot((CHI, LANES), lambda r, c: (r == c % CHI) & (c < 5 * CHI))
    loads[2].wait()
    left_proj = pl_ref[...].astype(jnp.float32)
    for k in range(CHI):
        z = f32dot(left_proj[:, CHI * k : CHI * k + CHI].astype(BF16), place_right)
        for h in range(2):
            plt[h, pl.ds(k, CHI, stride=CHI), :] = z[:, 128 * h : 128 * h + 128]
    acc_half[...] = jnp.zeros_like(acc_half)
    turn[...] = jnp.zeros_like(turn)
    summed[...] = jnp.zeros_like(summed)
    acc_whole[...] = jnp.zeros_like(acc_whole)
    await_copy(t1x, t1_got)
    mine, theirs = t1_ref[...].astype(jnp.float32), t1x[...].astype(jnp.float32)
    lower = jnp.where(core == 0, mine, theirs)
    upper = jnp.where(core == 0, theirs, mine)
    both = jnp.concatenate([lower, upper], axis=1)
    t1s[...] = jnp.concatenate(
        [both[:, TILE * t : TILE * t + TILE] for t in range(3)], axis=0
    ).astype(BF16)
    for t in range(3):
        t2p[LANES * t + TILE : LANES * t + LANES, :] = jnp.zeros(
            (LANES - TILE, GROUPS * LANES), BF16
        )

    def relay(dz):
        for cr in range(2):
            for a in FAR:
                await_piece(cr, dz, a, 0)
                pass_on(cr, dz, a, 0, to_b=FAR if dz else NEXT)

    def relay_near():
        for cr in range(2):
            for a in (0, *FAR):
                await_piece(cr, 0, a, 1)
                pass_on(cr, 0, a, 1, to_b=(3,))

    def collect(dz):
        for cr in range(2):
            await_copy(pieces.at[0 : 6 if dz else 4], piece_got.at[16 * cr + 12 + dz])

    def pack(g):
        w, height = row_window(g)
        row, run, skip = STARTS[g]
        for v in range(3):

            def hit(r, c):
                q = (r + 3 * v) % ROWS
                return c == (r + 3 * v) // ROWS * height + row - w + q + jnp.where(q < run, 0, skip)

            pick = one_hot((CHI, 6 * height), hit)
            for m in range(v, 12, 3):
                first = CHI * (m % 6) // ROWS
                source = pieces[first : first + 6, m // 6, w : w + height, :]
                source = source.reshape(6 * height, LANES)
                to = LANES * (m // 4) + CHI * (m % 4)
                t2p[to : to + CHI, LANES * g : LANES * g + LANES] = f32dot(pick, source).astype(BF16)

    weigh_some(2)
    relay(0)
    weigh_some(1)
    for cr in range(2):
        await_piece(cr, 1, 0, 0)
        pass_on(cr, 1, 0, 0, to_a=FAR, to_b=FAR)
    relay_near()
    weigh_some(1)
    relay(1)
    weigh_some(2)
    loads[3].wait()
    prt[...] = lax.dot_general(
        pr_ref[...], place_right, (((0,), (0,)), ((), ())), preferred_element_type=jnp.float32
    ).astype(BF16)
    collect(0)
    collect(1)

    p = lax.rem(i, 2)

    def diag(r):
        w = prt[pl.ds(pl.multiple_of(r * CHI, CHI), CHI), :]
        parts = [
            jnp.where((lane >= CHI * e) & (lane < CHI * (e + 1)), w, zero) for e in range(5)
        ]
        return jnp.concatenate(parts + [zero[:16]], axis=0)

    base = (48 * (1 - p), 24 * p)

    def project(slot, yb, total):
        r = lax.rem(24 * p + slot, CHI)
        for k in range(0, SLOTS_HERE, 4):
            weights = jnp.concatenate([diag(r + k + q) for q in range(4)], axis=0)
            left = [
                yb[:, CHI * (k + q) : CHI * (k + q + 1), :].reshape(GROUPS * CHI, LANES)
                for q in range(4)
            ]
            z = f32dot(jnp.concatenate(left, axis=1), weights)
            total[...] += z.reshape(GROUPS, CHI, LANES)

    def multiply(slot, yb, before=None):
        w = wf[pl.ds(pl.multiple_of(slot * CHI, CHI), STEP), :].astype(BF16)
        for g in range(GROUPS):
            if before is None:
                pack(g)
            elif g == 1:
                project(*before)
            yb[g] = f32dot(w, t2p[:, g * LANES : (g + 1) * LANES]).astype(BF16)

    def send_part(u, total):
        for z in range(4):
            for e in range(5):
                turn[z, CHI * e : CHI * e + CHI, 0:CHI] = total[z][:, CHI * e : CHI * e + CHI]
            at = CHI * SLOTS[z]
            turn[z, 5 * CHI : 6 * CHI, 0:CHI] = total[4][:, at : at + CHI]
        for z in range(4):
            for h in range(2):
                low = [turn[z, 72 * q + 36 * h : 72 * q + 36 * h + 40, :] for q in range(4)]
                part[u, z, h] = jnp.concatenate(
                    [low[q] + pltpu.roll(low[2 + q], 64, 1) for q in range(2)], axis=0
                ).astype(BF16)
        from_z[u, 4 * zh + zl] = part[u, zl, zh]
        for z, h, where in ring[1:]:
            send(2 + u, part.at[u, z, h], from_z.at[u, 4 * zh + zl], z_got.at[u], where)

    jobs = [(base[0] + SLOTS_HERE * k, acc_half) for k in range(2)]
    jobs += [(base[1] + SLOTS_HERE * k, acc_whole) for k in range(4)]
    before = None
    for k, (slot, total) in enumerate(jobs):
        yb = (yb0, yb1)[k % 2]
        multiply(slot, yb, before)
        before = (slot, yb, total)
        if k == 2:
            send_part(0, acc_half)
    project(*before)
    send_part(1, acc_whole)

    for u in range(2):
        await_copy(from_z.at[u, 0:7], z_got.at[u])
    for h in range(2):
        half, whole = [
            sum(from_z[u, 4 * h + z].astype(jnp.float32) for z in range(4)) for u in range(2)
        ]
        summed[2 * h, 0:80, :] = jnp.where(p == 0, whole, half)
        summed[2 * h + 1, 0:80, :] = jnp.where(p == 0, half, whole)
    wide = lax.broadcasted_iota(jnp.int32, (16, 128), 1)
    for yt in range(4):
        for xt in range(4):
            at = 40 * (yt % 2) + ROWS * xt
            sides = []
            for h in range(2):
                first, second = [summed[2 * h + f, at : at + 16, :] for f in range(2)]
                if yt < 2:
                    second = pltpu.roll(second, 64, 1)
                else:
                    first = pltpu.roll(first, 64, 1)
                sides.append(jnp.where(wide < 64, first, second))
            ready[4 * yt + xt] = jnp.concatenate(sides, axis=1).astype(BF16)

    spot = 4 * y + x
    for dy in range(4):
        for dx in range(4):
            if dy or dx:
                target = 4 * lax.rem(y + dy, 4) + lax.rem(x + dx, 4)
                where = {"row": row_of(0, dy, dx)}
                send(4, ready.at[target], arrived.at[spot], row_got, where)
    arrived[spot] = ready[spot]
    await_copy(arrived.at[0:15], row_got)
    blocks = []
    for t in range(16):
        source, h = 4 * (t // 4) + 2 * (t % 2), t // 2 % 2
        even, odd = [arrived[source + k].astype(jnp.float32) for k in range(2)]
        one, two = 128 * h, 128 * h + 64
        blocks.append(even[:, one : one + CHI])
        blocks.append(even[:, two : two + CHI] + odd[:, one : one + CHI])
        blocks.append(odd[:, two : two + CHI])
    out_ref[...] = jnp.concatenate(blocks, axis=1)[0:ROWS].astype(BF16)

    assert counts == [2 * (counts[0] // 2), 1, 7, 7, 15, 1], counts
    await_sent(0, pieces.at[0 : counts[0] // 2])
    await_sent(5, t2s.at[0])
    await_sent(1, t1x)
    await_sent(2, from_z.at[0, 0:7])
    await_sent(3, from_z.at[1, 0:7])
    await_sent(4, arrived.at[0:15])


def local(top_tensor, bottom_tensor, left_proj, right_proj):
    dma = pltpu.SemaphoreType.DMA
    return pl.pallas_call(
        kernel,
        out_shape=OUT,
        in_specs=[pl.BlockSpec(memory_space=pl.ANY)] * 4,
        out_specs=pl.BlockSpec(memory_space=pltpu.VMEM),
        scratch_shapes=[
            pltpu.VMEM((72, 288), BF16),
            pltpu.VMEM((ROWS, CHI * CHI), BF16),
            pltpu.VMEM((CHI, CHI * CHI), BF16),
            pltpu.VMEM((CHI, CHI * CHI), BF16),
            pltpu.VMEM((72, 288), BF16),
            pltpu.VMEM((2, 48, LANES), jnp.float32),
            pltpu.VMEM((2, 48, LANES), BF16),
            pltpu.VMEM((2, CHI * CHI, 128), jnp.float32),
            pltpu.VMEM((CHI * CHI, LANES), BF16),
            pltpu.VMEM((72 * CHI, 3 * LANES), jnp.float32),
            pltpu.VMEM((GROUPS, STEP, LANES), BF16),
            pltpu.VMEM((GROUPS, STEP, LANES), BF16),
            pltpu.VMEM((GROUPS, CHI, LANES), jnp.float32),
            pltpu.VMEM((GROUPS, CHI, LANES), jnp.float32),
            pltpu.VMEM((3 * 72, TILE), BF16),
            pltpu.VMEM((PEERS, 2, 48, LANES), BF16),
            pltpu.VMEM((3 * LANES, GROUPS * LANES), BF16),
            pltpu.VMEM((2, 4, 2, 80, 128), BF16),
            pltpu.VMEM((2, 8, 80, 128), BF16),
            pltpu.VMEM((4, 296, 128), jnp.float32),
            pltpu.VMEM((4, 88, 128), jnp.float32),
            pltpu.VMEM((16, 16, LANES), BF16),
            pltpu.VMEM((16, 16, LANES), BF16),
            dma((4,)),
            dma((6,)),
            dma,
            dma((32,)),
            dma((2,)),
            dma,
        ],
        compiler_params=pltpu.CompilerParams(
            vmem_limit_bytes=60 * 1024 * 1024, collective_id=0, has_side_effects=True
        ),
    )(top_tensor, bottom_tensor, left_proj.T, right_proj.T)


def solution(mesh):
    return jax.shard_map(
        local,
        mesh=mesh,
        in_specs=(P("row", "col"), P(("col", "row"), None), P(), P()),
        out_specs=P(("col", "row"), None),
        check_vma=False,
    )
```

```python
import jax
import jax.numpy as jnp
from jax import lax
from jax.experimental import pallas as pl
from jax.experimental.pallas import tpu as pltpu
from jax.sharding import PartitionSpec as P

CHI = 48
LANES = 256
ROWS = 9
TILE = 4 * CHI
GROUPS = 5
SLOTS_HERE = 12
STEP = SLOTS_HERE * CHI
OUT = pltpu.VMEM((9, 2304), jnp.bfloat16)
PEERS = 32
FAR = (3, 1, 2)
NEXT = (3, 1)
MESH = pl.DeviceIdType.MESH
BF16 = jnp.bfloat16
SLOTS = (0, 1, 3, 4)


STARTS = ((0, 9, 0), (16, 9, 0), (32, 9, 0), (9, 7, 9), (27, 5, 9))


def row_window(g):
    return ((0, 16), (16, 16), (32, 16), (0, 32), (16, 32))[g]


def f32dot(a, b):
    return jnp.dot(a, b, preferred_element_type=jnp.float32)


def one_hot(shape, hit):
    row = lax.broadcasted_iota(jnp.int32, shape, 0)
    col = lax.broadcasted_iota(jnp.int32, shape, 1)
    return jnp.where(hit(row, col), 1.0, 0.0).astype(BF16)


def kernel(
    t1_hbm, t2_hbm, pl_hbm, pr_hbm, out_ref,
    t1_ref, t2_ref, pl_ref, pr_ref, t1x, spread, t2s, plt, prt, wf, yb0, yb1, acc_half, acc_whole, t1s, pieces, t2p,
    part, from_z, turn, summed, ready, arrived,
    loaded, sent, t1_got, piece_got, z_got, row_got,
):
    i = lax.axis_index("row")
    j = lax.axis_index("col")
    x, zh, y = lax.rem(i, 4), lax.rem(i // 4, 2), i // 8
    core, zl = lax.rem(j, 2), j // 2
    other = 1 - core
    twin = 2 * zl + other
    def row_of(dz, dy, dx):
        return (lax.rem(y + dy, 4) * 2 + lax.rem(zh + dz, 2)) * 4 + lax.rem(x + dx, 4)

    ring = []
    for dz in range(2):
        for k in range(4):
            z = lax.rem(zl + k, 4)
            where = {"row": row_of(dz, 0, 0), "col": 2 * z + core}
            ring.append((z, lax.rem(zh + dz, 2), where))

    loads = []
    for k, (src, dst) in enumerate(
        ((t2_hbm, t2_ref), (t1_hbm, t1_ref), (pl_hbm, pl_ref), (pr_hbm, pr_ref))
    ):
        loads.append(pltpu.make_async_copy(src, dst, loaded.at[k]))
        loads[-1].start()
    barrier = pltpu.get_barrier_semaphore()
    near = [row_of(0, 0, k) for k in FAR] + [row_of(0, k, 0) for k in FAR]
    for peer in near:
        pl.semaphore_signal(barrier, inc=1, device_id={"row": peer}, device_id_type=MESH)
    pl.semaphore_signal(barrier, inc=1, device_id={"col": twin}, device_id_type=MESH)
    for _, _, where in ring[1:]:
        pl.semaphore_signal(barrier, inc=1, device_id=where, device_id_type=MESH)

    spread[...] = jnp.zeros_like(spread)
    loads[0].wait()
    t2 = t2_ref[...].astype(jnp.float32)
    for c in range(2):
        for z in range(4):
            at = 6 * CHI * (2 * z + c)
            slot = CHI * SLOTS[z]
            for g, left, lanes, width in ((z, at, 0, 5 * CHI), (4, at + 5 * CHI, slot, CHI)):
                row, run, skip = STARTS[g]
                value = t2[:, left : left + width]
                spread[c, row : row + run, lanes : lanes + width] = value[0:run]
                if run < ROWS:
                    to = row + run + skip
                    spread[c, to : to + ROWS - run, lanes : lanes + width] = value[run:ROWS]
    t2s[...] = spread[...].astype(BF16)
    pieces[i, core] = t2s[core]
    place_right = one_hot((CHI, LANES), lambda r, c: (r == c % CHI) & (c < 5 * CHI))
    loads[2].wait()
    left_proj = pl_ref[...].astype(jnp.float32)
    for k in range(CHI):
        z = f32dot(left_proj[:, CHI * k : CHI * k + CHI].astype(BF16), place_right)
        for h in range(2):
            plt[h, pl.ds(k, CHI, stride=CHI), :] = z[:, 128 * h : 128 * h + 128]
    loads[1].wait()

    pl.semaphore_wait(barrier, 6 + 1 + 7)

    counts = [0] * 6

    def remote(src, dst, kind, got, where):
        return pltpu.make_async_remote_copy(
            src_ref=src, dst_ref=dst, send_sem=sent.at[kind], recv_sem=got,
            device_id=where, device_id_type=MESH,
        )

    def send(kind, src, dst, got, where):
        remote(src, dst, kind, got, where).start()
        counts[kind] += 1

    def await_copy(ref, got):
        remote(ref, ref, 0, got, {"col": twin}).wait_recv()

    def await_sent(kind, ref):
        remote(ref, ref, kind, t1_got, {"col": twin}).wait_send()

    def place(cr, dz, a, b):
        return row_of(dz, b, a) if cr == 0 else row_of(dz, a, b)

    def block(cr):
        return core if cr == 0 else other

    def place_got(cr, dz, a, b):
        if b == 0:
            return 16 * cr + 8 * dz + a
        if b == 1 and dz == 0:
            return 16 * cr + 4 + a
        return 16 * cr + 12 + dz

    def pass_on(cr, dz, a, b, to_z=(), to_a=(), to_b=()):
        source, c = place(cr, dz, a, b), block(cr)
        own = cr == 0 and dz == 0 and a == 0 and b == 0
        src = t2s.at[core] if own else pieces.at[source, c]
        targets = [(place(cr, 1, 0, 0), place_got(cr, 1, 0, 0)) for _ in to_z]
        targets += [(place(cr, 0, t, 0), place_got(cr, dz, (a - t) % 4, b)) for t in to_a]
        targets += [(place(cr, 0, 0, t), place_got(cr, dz, a, (b - t) % 4)) for t in to_b]
        for target, got in targets:
            send(0, src, pieces.at[source, c], piece_got.at[got], {"row": target})

    def await_piece(cr, dz, a, b):
        await_copy(pieces.at[place(cr, dz, a, b), block(cr)], piece_got.at[place_got(cr, dz, a, b)])

    lane = lax.broadcasted_iota(jnp.int32, (CHI, LANES), 1)
    zero = jnp.zeros((CHI, LANES), BF16)
    swap = one_hot((192, 192), lambda r, c: (r // 8 == c % 24) & (r % 8 == c // 24))

    def weigh(ag, _):
        left = t1s[...]
        results = []
        for k in range(8):
            at = pl.multiple_of((8 * ag + k) * CHI, CHI)
            w = jnp.concatenate([plt[h, pl.ds(at, CHI), :] for h in range(2)], axis=1).astype(BF16)
            weights = jnp.concatenate(
                [jnp.where((lane >= CHI * m) & (lane < CHI * (m + 1)), w, zero) for m in range(4)], axis=0
            )
            results.append(f32dot(left, weights))
        for t in range(3):
            for s in range(3):
                at = 72 * t + 24 * s
                block = jnp.concatenate([r[at : at + 24] for r in results], axis=0).astype(BF16)
                turned = f32dot(swap, block)
                for q in range(24):
                    to = pl.multiple_of((24 * s + q) * CHI + 8 * ag, 8)
                    wf[pl.ds(to, 8), LANES * t : LANES * t + LANES] = turned[8 * q : 8 * q + 8]
        return _

    done = [0]

    def weigh_some(count):
        lax.fori_loop(done[0], done[0] + count, weigh, 0)
        done[0] += count

    send(5, t2s.at[other], pieces.at[i, core], piece_got.at[16], {"col": twin})
    send(1, t1_ref, t1x, t1_got, {"col": twin})
    pass_on(0, 0, 0, 0, to_z=(1,), to_a=FAR, to_b=NEXT)
    await_piece(1, 0, 0, 0)
    pass_on(1, 0, 0, 0, to_z=(1,), to_a=FAR, to_b=NEXT)

    acc_half[...] = jnp.zeros_like(acc_half)
    turn[...] = jnp.zeros_like(turn)
    summed[...] = jnp.zeros_like(summed)
    acc_whole[...] = jnp.zeros_like(acc_whole)
    await_copy(t1x, t1_got)
    mine, theirs = t1_ref[...].astype(jnp.float32), t1x[...].astype(jnp.float32)
    lower = jnp.where(core == 0, mine, theirs)
    upper = jnp.where(core == 0, theirs, mine)
    both = jnp.concatenate([lower, upper], axis=1)
    t1s[...] = jnp.concatenate(
        [both[:, TILE * t : TILE * t + TILE] for t in range(3)], axis=0
    ).astype(BF16)
    for t in range(3):
        t2p[LANES * t + TILE : LANES * t + LANES, :] = jnp.zeros(
            (LANES - TILE, GROUPS * LANES), BF16
        )

    def relay(dz):
        for cr in range(2):
            for a in FAR:
                await_piece(cr, dz, a, 0)
                pass_on(cr, dz, a, 0, to_b=FAR if dz else NEXT)

    def relay_near():
        for cr in range(2):
            for a in (0, *FAR):
                await_piece(cr, 0, a, 1)
                pass_on(cr, 0, a, 1, to_b=(3,))

    def collect(dz):
        for cr in range(2):
            await_copy(pieces.at[0 : 6 if dz else 4], piece_got.at[16 * cr + 12 + dz])

    def pack(g):
        w, height = row_window(g)
        row, run, skip = STARTS[g]
        for v in range(3):

            def hit(r, c):
                q = (r + 3 * v) % ROWS
                return c == (r + 3 * v) // ROWS * height + row - w + q + jnp.where(q < run, 0, skip)

            pick = one_hot((CHI, 6 * height), hit)
            for m in range(v, 12, 3):
                first = CHI * (m % 6) // ROWS
                source = pieces[first : first + 6, m // 6, w : w + height, :]
                source = source.reshape(6 * height, LANES)
                to = LANES * (m // 4) + CHI * (m % 4)
                t2p[to : to + CHI, LANES * g : LANES * g + LANES] = f32dot(pick, source).astype(BF16)

    weigh_some(1)
    relay(0)
    for cr in range(2):
        await_piece(cr, 1, 0, 0)
        pass_on(cr, 1, 0, 0, to_a=FAR, to_b=FAR)
    relay_near()
    weigh_some(3)
    relay(1)
    weigh_some(2)
    loads[3].wait()
    prt[...] = lax.dot_general(
        pr_ref[...], place_right, (((0,), (0,)), ((), ())), preferred_element_type=jnp.float32
    ).astype(BF16)
    collect(0)
    collect(1)

    p = lax.rem(i, 2)

    def diag(r):
        w = prt[pl.ds(pl.multiple_of(r * CHI, CHI), CHI), :]
        parts = [
            jnp.where((lane >= CHI * e) & (lane < CHI * (e + 1)), w, zero) for e in range(5)
        ]
        return jnp.concatenate(parts + [zero[:16]], axis=0)

    base = (48 * (1 - p), 24 * p)

    def project(slot, yb, total):
        r = lax.rem(24 * p + slot, CHI)
        for k in range(0, SLOTS_HERE, 4):
            weights = jnp.concatenate([diag(r + k + q) for q in range(4)], axis=0)
            left = [
                yb[:, CHI * (k + q) : CHI * (k + q + 1), :].reshape(GROUPS * CHI, LANES)
                for q in range(4)
            ]
            z = f32dot(jnp.concatenate(left, axis=1), weights)
            total[...] += z.reshape(GROUPS, CHI, LANES)

    def multiply(slot, yb, before=None):
        w = wf[pl.ds(pl.multiple_of(slot * CHI, CHI), STEP), :].astype(BF16)
        for g in range(GROUPS):
            if before is None:
                pack(g)
            elif g == 1:
                project(*before)
            yb[g] = f32dot(w, t2p[:, g * LANES : (g + 1) * LANES]).astype(BF16)

    def send_part(u, total):
        for z in range(4):
            for e in range(5):
                turn[z, CHI * e : CHI * e + CHI, 0:CHI] = total[z][:, CHI * e : CHI * e + CHI]
            at = CHI * SLOTS[z]
            turn[z, 5 * CHI : 6 * CHI, 0:CHI] = total[4][:, at : at + CHI]
        for z in range(4):
            for h in range(2):
                low = [turn[z, 72 * q + 36 * h : 72 * q + 36 * h + 40, :] for q in range(4)]
                part[u, z, h] = jnp.concatenate(
                    [low[q] + pltpu.roll(low[2 + q], 64, 1) for q in range(2)], axis=0
                ).astype(BF16)
        from_z[u, 4 * zh + zl] = part[u, zl, zh]
        for z, h, where in ring[1:]:
            send(2 + u, part.at[u, z, h], from_z.at[u, 4 * zh + zl], z_got.at[u], where)

    jobs = [(base[0] + SLOTS_HERE * k, acc_half) for k in range(2)]
    jobs += [(base[1] + SLOTS_HERE * k, acc_whole) for k in range(4)]
    before = None
    for k, (slot, total) in enumerate(jobs):
        yb = (yb0, yb1)[k % 2]
        multiply(slot, yb, before)
        before = (slot, yb, total)
        if k == 2:
            send_part(0, acc_half)
    project(*before)
    send_part(1, acc_whole)

    for u in range(2):
        await_copy(from_z.at[u, 0:7], z_got.at[u])
    for h in range(2):
        half, whole = [
            sum(from_z[u, 4 * h + z].astype(jnp.float32) for z in range(4)) for u in range(2)
        ]
        summed[2 * h, 0:80, :] = jnp.where(p == 0, whole, half)
        summed[2 * h + 1, 0:80, :] = jnp.where(p == 0, half, whole)
    wide = lax.broadcasted_iota(jnp.int32, (16, 128), 1)
    for yt in range(4):
        for xt in range(4):
            at = 40 * (yt % 2) + ROWS * xt
            sides = []
            for h in range(2):
                first, second = [summed[2 * h + f, at : at + 16, :] for f in range(2)]
                if yt < 2:
                    second = pltpu.roll(second, 64, 1)
                else:
                    first = pltpu.roll(first, 64, 1)
                sides.append(jnp.where(wide < 64, first, second))
            ready[4 * yt + xt] = jnp.concatenate(sides, axis=1).astype(BF16)

    spot = 4 * y + x
    for dy in range(4):
        for dx in range(4):
            if dy or dx:
                target = 4 * lax.rem(y + dy, 4) + lax.rem(x + dx, 4)
                where = {"row": row_of(0, dy, dx)}
                send(4, ready.at[target], arrived.at[spot], row_got, where)
    arrived[spot] = ready[spot]
    await_copy(arrived.at[0:15], row_got)
    blocks = []
    for t in range(16):
        source, h = 4 * (t // 4) + 2 * (t % 2), t // 2 % 2
        even, odd = [arrived[source + k].astype(jnp.float32) for k in range(2)]
        one, two = 128 * h, 128 * h + 64
        blocks.append(even[:, one : one + CHI])
        blocks.append(even[:, two : two + CHI] + odd[:, one : one + CHI])
        blocks.append(odd[:, two : two + CHI])
    out_ref[...] = jnp.concatenate(blocks, axis=1)[0:ROWS].astype(BF16)

    assert counts == [2 * (counts[0] // 2), 1, 7, 7, 15, 1], counts
    await_sent(0, pieces.at[0 : counts[0] // 2])
    await_sent(5, t2s.at[0])
    await_sent(1, t1x)
    await_sent(2, from_z.at[0, 0:7])
    await_sent(3, from_z.at[1, 0:7])
    await_sent(4, arrived.at[0:15])


def local(top_tensor, bottom_tensor, left_proj, right_proj):
    dma = pltpu.SemaphoreType.DMA
    return pl.pallas_call(
        kernel,
        out_shape=OUT,
        in_specs=[pl.BlockSpec(memory_space=pl.ANY)] * 4,
        out_specs=pl.BlockSpec(memory_space=pltpu.VMEM),
        scratch_shapes=[
            pltpu.VMEM((72, 288), BF16),
            pltpu.VMEM((ROWS, CHI * CHI), BF16),
            pltpu.VMEM((CHI, CHI * CHI), BF16),
            pltpu.VMEM((CHI, CHI * CHI), BF16),
            pltpu.VMEM((72, 288), BF16),
            pltpu.VMEM((2, 48, LANES), jnp.float32),
            pltpu.VMEM((2, 48, LANES), BF16),
            pltpu.VMEM((2, CHI * CHI, 128), jnp.float32),
            pltpu.VMEM((CHI * CHI, LANES), BF16),
            pltpu.VMEM((72 * CHI, 3 * LANES), jnp.float32),
            pltpu.VMEM((GROUPS, STEP, LANES), BF16),
            pltpu.VMEM((GROUPS, STEP, LANES), BF16),
            pltpu.VMEM((GROUPS, CHI, LANES), jnp.float32),
            pltpu.VMEM((GROUPS, CHI, LANES), jnp.float32),
            pltpu.VMEM((3 * 72, TILE), BF16),
            pltpu.VMEM((PEERS, 2, 48, LANES), BF16),
            pltpu.VMEM((3 * LANES, GROUPS * LANES), BF16),
            pltpu.VMEM((2, 4, 2, 80, 128), BF16),
            pltpu.VMEM((2, 8, 80, 128), BF16),
            pltpu.VMEM((4, 296, 128), jnp.float32),
            pltpu.VMEM((4, 88, 128), jnp.float32),
            pltpu.VMEM((16, 16, LANES), BF16),
            pltpu.VMEM((16, 16, LANES), BF16),
            dma((4,)),
            dma((6,)),
            dma,
            dma((32,)),
            dma((2,)),
            dma,
        ],
        compiler_params=pltpu.CompilerParams(
            vmem_limit_bytes=60 * 1024 * 1024, collective_id=0, has_side_effects=True
        ),
    )(top_tensor, bottom_tensor, left_proj.T, right_proj.T)


def solution(mesh):
    return jax.shard_map(
        local,
        mesh=mesh,
        in_specs=(P("row", "col"), P(("col", "row"), None), P(), P()),
        out_specs=P(("col", "row"), None),
        check_vma=False,
    )
```

```python
import jax
import jax.numpy as jnp
from jax import lax
from jax.experimental import pallas as pl
from jax.experimental.pallas import tpu as pltpu
from jax.sharding import PartitionSpec as P

CHI = 48
LANES = 256
ROWS = 9
TILE = 4 * CHI
GROUPS = 5
SLOTS_HERE = 12
STEP = SLOTS_HERE * CHI
OUT = pltpu.VMEM((9, 2304), jnp.bfloat16)
PEERS = 32
FAR = (3, 1, 2)
NEXT = (3, 1)
MESH = pl.DeviceIdType.MESH
BF16 = jnp.bfloat16
SLOTS = (0, 1, 3, 4)


STARTS = ((0, 9, 0), (16, 9, 0), (32, 9, 0), (9, 7, 9), (27, 5, 9))


def row_window(g):
    return ((0, 16), (16, 16), (32, 16), (0, 32), (16, 32))[g]


def f32dot(a, b):
    return jnp.dot(a, b, preferred_element_type=jnp.float32)


def one_hot(shape, hit):
    row = lax.broadcasted_iota(jnp.int32, shape, 0)
    col = lax.broadcasted_iota(jnp.int32, shape, 1)
    return jnp.where(hit(row, col), 1.0, 0.0).astype(BF16)


def kernel(
    t1_hbm, t2_hbm, pl_hbm, pr_hbm, out_ref,
    t1_ref, t2_ref, pl_ref, pr_ref, t1x, spread, t2s, plt, prt, wf, yb0, yb1, acc_half, acc_whole, t1s, pieces, t2p,
    part, from_z, turn, summed, ready, arrived,
    loaded, sent, t1_got, piece_got, z_got, row_got,
):
    i = lax.axis_index("row")
    j = lax.axis_index("col")
    x, zh, y = lax.rem(i, 4), lax.rem(i // 4, 2), i // 8
    core, zl = lax.rem(j, 2), j // 2
    other = 1 - core
    twin = 2 * zl + other
    def row_of(dz, dy, dx):
        return (lax.rem(y + dy, 4) * 2 + lax.rem(zh + dz, 2)) * 4 + lax.rem(x + dx, 4)

    ring = []
    for dz in range(2):
        for k in range(4):
            z = lax.rem(zl + k, 4)
            where = {"row": row_of(dz, 0, 0), "col": 2 * z + core}
            ring.append((z, lax.rem(zh + dz, 2), where))

    loads = []
    for k, (src, dst) in enumerate(
        ((t2_hbm, t2_ref), (t1_hbm, t1_ref), (pl_hbm, pl_ref), (pr_hbm, pr_ref))
    ):
        loads.append(pltpu.make_async_copy(src, dst, loaded.at[k]))
        loads[-1].start()
    barrier = pltpu.get_barrier_semaphore()
    near = [row_of(0, 0, k) for k in FAR] + [row_of(0, k, 0) for k in FAR]
    for peer in near:
        pl.semaphore_signal(barrier, inc=1, device_id={"row": peer}, device_id_type=MESH)
    pl.semaphore_signal(barrier, inc=1, device_id={"col": twin}, device_id_type=MESH)
    for _, _, where in ring[1:]:
        pl.semaphore_signal(barrier, inc=1, device_id=where, device_id_type=MESH)

    spread[...] = jnp.zeros_like(spread)
    loads[0].wait()
    t2 = t2_ref[...].astype(jnp.float32)
    for c in range(2):
        for z in range(4):
            at = 6 * CHI * (2 * z + c)
            slot = CHI * SLOTS[z]
            for g, left, lanes, width in ((z, at, 0, 5 * CHI), (4, at + 5 * CHI, slot, CHI)):
                row, run, skip = STARTS[g]
                value = t2[:, left : left + width]
                spread[c, row : row + run, lanes : lanes + width] = value[0:run]
                if run < ROWS:
                    to = row + run + skip
                    spread[c, to : to + ROWS - run, lanes : lanes + width] = value[run:ROWS]
    t2s[...] = spread[...].astype(BF16)
    pieces[i, core] = t2s[core]
    place_right = one_hot((CHI, LANES), lambda r, c: (r == c % CHI) & (c < 5 * CHI))
    loads[2].wait()
    left_proj = pl_ref[...].astype(jnp.float32)
    for k in range(CHI):
        z = f32dot(left_proj[:, CHI * k : CHI * k + CHI].astype(BF16), place_right)
        for h in range(2):
            plt[h, pl.ds(k, CHI, stride=CHI), :] = z[:, 128 * h : 128 * h + 128]
    loads[1].wait()

    pl.semaphore_wait(barrier, 6 + 1 + 7)

    counts = [0] * 6

    def remote(src, dst, kind, got, where):
        return pltpu.make_async_remote_copy(
            src_ref=src, dst_ref=dst, send_sem=sent.at[kind], recv_sem=got,
            device_id=where, device_id_type=MESH,
        )

    def send(kind, src, dst, got, where):
        remote(src, dst, kind, got, where).start()
        counts[kind] += 1

    def await_copy(ref, got):
        remote(ref, ref, 0, got, {"col": twin}).wait_recv()

    def await_sent(kind, ref):
        remote(ref, ref, kind, t1_got, {"col": twin}).wait_send()

    def place(cr, dz, a, b):
        return row_of(dz, b, a) if cr == 0 else row_of(dz, a, b)

    def block(cr):
        return core if cr == 0 else other

    def place_got(cr, dz, a, b):
        if b == 0:
            return 16 * cr + 8 * dz + a
        if b == 1 and dz == 0:
            return 16 * cr + 4 + a
        return 16 * cr + 12 + dz

    def pass_on(cr, dz, a, b, to_z=(), to_a=(), to_b=()):
        source, c = place(cr, dz, a, b), block(cr)
        own = cr == 0 and dz == 0 and a == 0 and b == 0
        src = t2s.at[core] if own else pieces.at[source, c]
        targets = [(place(cr, 1, 0, 0), place_got(cr, 1, 0, 0)) for _ in to_z]
        targets += [(place(cr, 0, t, 0), place_got(cr, dz, (a - t) % 4, b)) for t in to_a]
        targets += [(place(cr, 0, 0, t), place_got(cr, dz, a, (b - t) % 4)) for t in to_b]
        for target, got in targets:
            send(0, src, pieces.at[source, c], piece_got.at[got], {"row": target})

    def await_piece(cr, dz, a, b):
        await_copy(pieces.at[place(cr, dz, a, b), block(cr)], piece_got.at[place_got(cr, dz, a, b)])

    lane = lax.broadcasted_iota(jnp.int32, (CHI, LANES), 1)
    zero = jnp.zeros((CHI, LANES), BF16)
    swap = one_hot((192, 192), lambda r, c: (r // 8 == c % 24) & (r % 8 == c // 24))

    def weigh(ag, _):
        left = t1s[...]
        results = []
        for k in range(8):
            at = pl.multiple_of((8 * ag + k) * CHI, CHI)
            w = jnp.concatenate([plt[h, pl.ds(at, CHI), :] for h in range(2)], axis=1).astype(BF16)
            weights = jnp.concatenate(
                [jnp.where((lane >= CHI * m) & (lane < CHI * (m + 1)), w, zero) for m in range(4)], axis=0
            )
            results.append(f32dot(left, weights))
        for t in range(3):
            for s in range(3):
                at = 72 * t + 24 * s
                block = jnp.concatenate([r[at : at + 24] for r in results], axis=0).astype(BF16)
                turned = f32dot(swap, block)
                for q in range(24):
                    to = pl.multiple_of((24 * s + q) * CHI + 8 * ag, 8)
                    wf[pl.ds(to, 8), LANES * t : LANES * t + LANES] = turned[8 * q : 8 * q + 8]
        return _

    done = [0]

    def weigh_some(count):
        lax.fori_loop(done[0], done[0] + count, weigh, 0)
        done[0] += count

    send(5, t2s.at[other], pieces.at[i, core], piece_got.at[16], {"col": twin})
    send(1, t1_ref, t1x, t1_got, {"col": twin})
    pass_on(0, 0, 0, 0, to_z=(1,), to_a=FAR, to_b=NEXT)
    await_piece(1, 0, 0, 0)
    pass_on(1, 0, 0, 0, to_z=(1,), to_a=FAR, to_b=NEXT)

    await_copy(t1x, t1_got)
    mine, theirs = t1_ref[...].astype(jnp.float32), t1x[...].astype(jnp.float32)
    lower = jnp.where(core == 0, mine, theirs)
    upper = jnp.where(core == 0, theirs, mine)
    both = jnp.concatenate([lower, upper], axis=1)
    t1s[...] = jnp.concatenate(
        [both[:, TILE * t : TILE * t + TILE] for t in range(3)], axis=0
    ).astype(BF16)
    def relay(dz):
        for cr in range(2):
            for a in FAR:
                await_piece(cr, dz, a, 0)
                pass_on(cr, dz, a, 0, to_b=FAR if dz else NEXT)

    def relay_near():
        for cr in range(2):
            for a in (0, *FAR):
                await_piece(cr, 0, a, 1)
                pass_on(cr, 0, a, 1, to_b=(3,))

    def collect(dz):
        for cr in range(2):
            await_copy(pieces.at[0 : 6 if dz else 4], piece_got.at[16 * cr + 12 + dz])

    def pack(g):
        w, height = row_window(g)
        row, run, skip = STARTS[g]
        for v in range(3):

            def hit(r, c):
                q = (r + 3 * v) % ROWS
                return c == (r + 3 * v) // ROWS * height + row - w + q + jnp.where(q < run, 0, skip)

            pick = one_hot((CHI, 6 * height), hit)
            for m in range(v, 12, 3):
                first = CHI * (m % 6) // ROWS
                source = pieces[first : first + 6, m // 6, w : w + height, :]
                source = source.reshape(6 * height, LANES)
                to = LANES * (m // 4) + CHI * (m % 4)
                t2p[to : to + CHI, LANES * g : LANES * g + LANES] = f32dot(pick, source).astype(BF16)

    weigh_some(1)
    relay(0)
    for cr in range(2):
        await_piece(cr, 1, 0, 0)
        pass_on(cr, 1, 0, 0, to_a=FAR, to_b=FAR)
    relay_near()
    weigh_some(3)
    relay(1)
    weigh_some(2)
    acc_half[...] = jnp.zeros_like(acc_half)
    turn[...] = jnp.zeros_like(turn)
    summed[...] = jnp.zeros_like(summed)
    acc_whole[...] = jnp.zeros_like(acc_whole)
    for t in range(3):
        t2p[LANES * t + TILE : LANES * t + LANES, :] = jnp.zeros(
            (LANES - TILE, GROUPS * LANES), BF16
        )
    loads[3].wait()
    prt[...] = lax.dot_general(
        pr_ref[...], place_right, (((0,), (0,)), ((), ())), preferred_element_type=jnp.float32
    ).astype(BF16)
    collect(0)
    collect(1)

    p = lax.rem(i, 2)

    def diag(r):
        w = prt[pl.ds(pl.multiple_of(r * CHI, CHI), CHI), :]
        parts = [
            jnp.where((lane >= CHI * e) & (lane < CHI * (e + 1)), w, zero) for e in range(5)
        ]
        return jnp.concatenate(parts + [zero[:16]], axis=0)

    base = (48 * (1 - p), 24 * p)

    def project(slot, yb, total):
        r = lax.rem(24 * p + slot, CHI)
        for k in range(0, SLOTS_HERE, 4):
            weights = jnp.concatenate([diag(r + k + q) for q in range(4)], axis=0)
            left = [
                yb[:, CHI * (k + q) : CHI * (k + q + 1), :].reshape(GROUPS * CHI, LANES)
                for q in range(4)
            ]
            z = f32dot(jnp.concatenate(left, axis=1), weights)
            total[...] += z.reshape(GROUPS, CHI, LANES)

    def multiply(slot, yb, before=None):
        w = wf[pl.ds(pl.multiple_of(slot * CHI, CHI), STEP), :].astype(BF16)
        for g in range(GROUPS):
            if before is None:
                pack(g)
            elif g == 1:
                project(*before)
            yb[g] = f32dot(w, t2p[:, g * LANES : (g + 1) * LANES]).astype(BF16)

    def send_part(u, total):
        for z in range(4):
            for e in range(5):
                turn[z, CHI * e : CHI * e + CHI, 0:CHI] = total[z][:, CHI * e : CHI * e + CHI]
            at = CHI * SLOTS[z]
            turn[z, 5 * CHI : 6 * CHI, 0:CHI] = total[4][:, at : at + CHI]
        for z in range(4):
            for h in range(2):
                low = [turn[z, 72 * q + 36 * h : 72 * q + 36 * h + 40, :] for q in range(4)]
                part[u, z, h] = jnp.concatenate(
                    [low[q] + pltpu.roll(low[2 + q], 64, 1) for q in range(2)], axis=0
                ).astype(BF16)
        from_z[u, 4 * zh + zl] = part[u, zl, zh]
        for z, h, where in ring[1:]:
            send(2 + u, part.at[u, z, h], from_z.at[u, 4 * zh + zl], z_got.at[u], where)

    jobs = [(base[0] + SLOTS_HERE * k, acc_half) for k in range(2)]
    jobs += [(base[1] + SLOTS_HERE * k, acc_whole) for k in range(4)]
    before = None
    for k, (slot, total) in enumerate(jobs):
        yb = (yb0, yb1)[k % 2]
        multiply(slot, yb, before)
        before = (slot, yb, total)
        if k == 2:
            send_part(0, acc_half)
    project(*before)
    send_part(1, acc_whole)

    for u in range(2):
        await_copy(from_z.at[u, 0:7], z_got.at[u])
    for h in range(2):
        half, whole = [
            sum(from_z[u, 4 * h + z].astype(jnp.float32) for z in range(4)) for u in range(2)
        ]
        summed[2 * h, 0:80, :] = jnp.where(p == 0, whole, half)
        summed[2 * h + 1, 0:80, :] = jnp.where(p == 0, half, whole)
    wide = lax.broadcasted_iota(jnp.int32, (16, 128), 1)
    for yt in range(4):
        for xt in range(4):
            at = 40 * (yt % 2) + ROWS * xt
            sides = []
            for h in range(2):
                first, second = [summed[2 * h + f, at : at + 16, :] for f in range(2)]
                if yt < 2:
                    second = pltpu.roll(second, 64, 1)
                else:
                    first = pltpu.roll(first, 64, 1)
                sides.append(jnp.where(wide < 64, first, second))
            ready[4 * yt + xt] = jnp.concatenate(sides, axis=1).astype(BF16)

    spot = 4 * y + x
    for dy in range(4):
        for dx in range(4):
            if dy or dx:
                target = 4 * lax.rem(y + dy, 4) + lax.rem(x + dx, 4)
                where = {"row": row_of(0, dy, dx)}
                send(4, ready.at[target], arrived.at[spot], row_got, where)
    arrived[spot] = ready[spot]
    await_copy(arrived.at[0:15], row_got)
    blocks = []
    for t in range(16):
        source, h = 4 * (t // 4) + 2 * (t % 2), t // 2 % 2
        even, odd = [arrived[source + k].astype(jnp.float32) for k in range(2)]
        one, two = 128 * h, 128 * h + 64
        blocks.append(even[:, one : one + CHI])
        blocks.append(even[:, two : two + CHI] + odd[:, one : one + CHI])
        blocks.append(odd[:, two : two + CHI])
    out_ref[...] = jnp.concatenate(blocks, axis=1)[0:ROWS].astype(BF16)

    assert counts == [2 * (counts[0] // 2), 1, 7, 7, 15, 1], counts
    await_sent(0, pieces.at[0 : counts[0] // 2])
    await_sent(5, t2s.at[0])
    await_sent(1, t1x)
    await_sent(2, from_z.at[0, 0:7])
    await_sent(3, from_z.at[1, 0:7])
    await_sent(4, arrived.at[0:15])


def local(top_tensor, bottom_tensor, left_proj, right_proj):
    dma = pltpu.SemaphoreType.DMA
    return pl.pallas_call(
        kernel,
        out_shape=OUT,
        in_specs=[pl.BlockSpec(memory_space=pl.ANY)] * 4,
        out_specs=pl.BlockSpec(memory_space=pltpu.VMEM),
        scratch_shapes=[
            pltpu.VMEM((72, 288), BF16),
            pltpu.VMEM((ROWS, CHI * CHI), BF16),
            pltpu.VMEM((CHI, CHI * CHI), BF16),
            pltpu.VMEM((CHI, CHI * CHI), BF16),
            pltpu.VMEM((72, 288), BF16),
            pltpu.VMEM((2, 48, LANES), jnp.float32),
            pltpu.VMEM((2, 48, LANES), BF16),
            pltpu.VMEM((2, CHI * CHI, 128), jnp.float32),
            pltpu.VMEM((CHI * CHI, LANES), BF16),
            pltpu.VMEM((72 * CHI, 3 * LANES), jnp.float32),
            pltpu.VMEM((GROUPS, STEP, LANES), BF16),
            pltpu.VMEM((GROUPS, STEP, LANES), BF16),
            pltpu.VMEM((GROUPS, CHI, LANES), jnp.float32),
            pltpu.VMEM((GROUPS, CHI, LANES), jnp.float32),
            pltpu.VMEM((3 * 72, TILE), BF16),
            pltpu.VMEM((PEERS, 2, 48, LANES), BF16),
            pltpu.VMEM((3 * LANES, GROUPS * LANES), BF16),
            pltpu.VMEM((2, 4, 2, 80, 128), BF16),
            pltpu.VMEM((2, 8, 80, 128), BF16),
            pltpu.VMEM((4, 296, 128), jnp.float32),
            pltpu.VMEM((4, 88, 128), jnp.float32),
            pltpu.VMEM((16, 16, LANES), BF16),
            pltpu.VMEM((16, 16, LANES), BF16),
            dma((4,)),
            dma((6,)),
            dma,
            dma((32,)),
            dma((2,)),
            dma,
        ],
        compiler_params=pltpu.CompilerParams(
            vmem_limit_bytes=60 * 1024 * 1024, collective_id=0, has_side_effects=True
        ),
    )(top_tensor, bottom_tensor, left_proj.T, right_proj.T)


def solution(mesh):
    return jax.shard_map(
        local,
        mesh=mesh,
        in_specs=(P("row", "col"), P(("col", "row"), None), P(), P()),
        out_specs=P(("col", "row"), None),
        check_vma=False,
    )
```
